32 devices in a mesh: tm: 2 (over x), slab: 16 (over z, y, core).
Axes of the slice: x: 2, y: 2, z: 4, core: 2. Of those that a mesh axis runs over, the one named last changes fastest.
Arguments:
- volumes: bfloat16 [16, 1024, 64, 128], P('tm', 'slab'), parts along dimension 0, may hold values from -6 to 6
- pair_fields: int32 [8, 128], P(None, ('tm', 'slab')), parts along dimension 1, may hold values from -16 to 64, as said below
- pair_counts: int32 [32], P(('tm', 'slab')), parts along dimension 0, may hold values from 1 to 4, as said below
Outputs:
- correlation: float32 [128, 512], P(('tm', 'slab')), parts along dimension 0
- shifts: float32 [3, 128], P(None, ('tm', 'slab')), parts along dimension 1
- normal_sums: float32 [16, 4, 4], P('tm'), parts along dimension 0
- rhs_sums: float32 [16, 4, 3], P('tm'), parts along dimension 0
The draws below stay inside these ranges and needn't reach their ends.
There are 2 independent parts, one for each index of `tm`. The reference program is written for one: setup_inputs(seed, part) draws one part's arguments, and reference() takes and returns one part's arrays. A program takes and returns all parts, laid end to end along the dimension named above; each array names one. Nothing has to cross between parts.
Inputs may be any that keep to these rules, and one draw needn't show every extreme that they name: `pair_fields`: column p belongs to slab p // 4. Rows: first view; x anchor of its block (0 to 64); second view, the first plus or minus one modulo 8; slab offset of the second block (-1, 0 or 1, never leading outside the volume; 0 in dead columns); x anchor of the second block (0 to 64); window offsets along z, y, x (-16 to 8). Among one slab's live pairs at most 2 have slab offset 1 and at most 2 have -1; in every draw some slab has exactly 2 of each. The first pair of the first slab has slab offset 1 and the first pair of the last slab has -1. `pair_counts`: the live pairs of a slab fill its first slots; in every draw some slab has 4.
All inputs are finite; a program needn't handle non-finite values.
Results may differ from the reference program's by a relative error of at most 0.0003.
Values may be sent and summed in bfloat16 or wider, within the bound.
A program may use at most 128 MiB of HBM per device.

```python
import jax
import jax.numpy as jnp
from jax import lax

VIEWS = 8
B = 64
WIN = 8
CAP = 4
NBR = 2
N_SLAB = 16


def pair_plan(key):
    base = jax.random.fold_in(key, 917)
    keys = jax.random.split(base, 9)
    slab_ids = jnp.arange(N_SLAB, dtype=jnp.int32)
    full_slab = jax.random.randint(keys[0], (), 1, N_SLAB - 1)
    heavy = jax.random.randint(keys[1], (N_SLAB,), 0, 8) == 0
    light = jax.random.randint(keys[2], (N_SLAB,), 1, CAP // 2 + 1)
    counts = jnp.where(heavy | (slab_ids == full_slab), CAP, light).astype(jnp.int32)
    pair_total = N_SLAB * CAP
    owner = jnp.arange(pair_total, dtype=jnp.int32) // CAP
    slot_index = jnp.arange(pair_total, dtype=jnp.int32) % CAP
    first_view = jax.random.randint(keys[3], (pair_total,), 0, VIEWS)
    step_sign = 2 * jax.random.randint(keys[4], (pair_total,), 0, 2) - 1
    second_view = jnp.mod(first_view + step_sign, VIEWS)
    first_x = jax.random.randint(keys[5], (pair_total,), 0, B + 1)
    second_x = jax.random.randint(keys[6], (pair_total,), 0, B + 1)
    offsets = jax.random.randint(keys[7], (3, pair_total), -2 * WIN, WIN + 1)
    direction = jax.random.randint(keys[8], (pair_total,), -1, 2)
    live = slot_index < counts[owner]
    direction = jnp.where(live, direction, 0)
    direction = jnp.where((owner == 0) & (direction < 0), 0, direction)
    direction = jnp.where((owner == N_SLAB - 1) & (direction > 0), 0, direction)
    direction = jnp.where((owner == 0) & (slot_index == 0), 1, direction)
    direction = jnp.where((owner == N_SLAB - 1) & (slot_index == 0), -1, direction)
    grid = direction.reshape(N_SLAB, CAP)
    up_rank = jnp.cumsum((grid == 1).astype(jnp.int32), axis=1)
    down_rank = jnp.cumsum((grid == -1).astype(jnp.int32), axis=1)
    grid = jnp.where((grid == 1) & (up_rank > NBR), 0, grid)
    grid = jnp.where((grid == -1) & (down_rank > NBR), 0, grid)
    slot_ids = jnp.arange(CAP, dtype=jnp.int32)
    forced = jnp.where(slot_ids < NBR, 1, jnp.where(slot_ids < 2 * NBR, -1, 0))
    grid = jnp.where((slab_ids == full_slab)[:, None], forced[None, :], grid)
    direction = grid.reshape(-1)
    fields = jnp.stack([first_view, first_x, second_view, direction, second_x, offsets[0], offsets[1], offsets[2]]).astype(jnp.int32)
    return (fields, counts)


def draw_pair_fields(key, part):
    return pair_plan(key)[0]


def draw_pair_counts(key, part):
    return pair_plan(key)[1]


def block_levels(rng, dims, shards, least, top_value):
    level, own = 1.0, jax.random.fold_in(rng, 6)
    for position, blocks in shards:
        draws = jnp.exp(jax.random.uniform(jax.random.fold_in(own, position), (blocks,), jnp.float32, least / len(shards), top_value / len(shards)))
        level = level * jnp.repeat(draws, dims[position] // blocks).reshape([-1 if axis == position else 1 for axis in range(len(dims))])
    return level


def centred(key, extent, scale, limit, cuts=(), held_as=jnp.bfloat16):
    loudness = block_levels(key, extent, cuts, -0.22, 0.18) if cuts else 1.0
    entries = jax.random.normal(key, extent, jnp.float32) * scale * loudness
    return jnp.minimum(jnp.maximum(entries, -limit), limit).astype(held_as)


def setup_inputs(seed: int = 0, part: int = 0) -> dict:
    arg_keys = jax.random.split(jax.random.key(seed), 4)
    own_keys = jax.random.split(jax.random.fold_in(arg_keys[3], part), 4)
    return {
        "volumes": centred(own_keys[0], (VIEWS, B * N_SLAB, B, 2 * B), 1.0, 6.0, ((1, 16),)),
        "pair_fields": draw_pair_fields(jax.random.fold_in(jax.random.fold_in(arg_keys[3], part), 71), part),
        "pair_counts": draw_pair_counts(jax.random.fold_in(jax.random.fold_in(arg_keys[3], part), 71), part),
    }


EPSILON = 1e-6


def reference(volumes, pair_fields, pair_counts):
    pair_total = CAP * N_SLAB
    window_steps = jnp.arange(WIN, dtype=jnp.int32)
    view_ids = jnp.arange(VIEWS, dtype=jnp.int32)

    def one_pair(pair_index):
        slab_pos = (pair_index // CAP).astype(jnp.int32)
        slot_index = pair_index % CAP
        column = pair_fields[:, pair_index]
        live_mask = (slot_index < pair_counts[slab_pos]).astype(jnp.float32)
        start_a = (slab_pos * B).astype(jnp.int32)
        start_b = ((slab_pos + column[3]) * B).astype(jnp.int32)
        block_a = lax.dynamic_slice(volumes, (column[0].astype(jnp.int32), start_a, jnp.zeros((), jnp.int32), column[1].astype(jnp.int32)), (1, B, B, B))[0].astype(jnp.float32)
        block_b = lax.dynamic_slice(volumes, (column[2].astype(jnp.int32), start_b, jnp.zeros((), jnp.int32), column[4].astype(jnp.int32)), (1, B, B, B))[0].astype(jnp.float32)
        spec_a = jnp.fft.fftn(block_a)
        spec_b = jnp.fft.fftn(block_b)
        cross_term = spec_a * jnp.conj(spec_b)
        magnitude = jnp.abs(cross_term)
        ratio_term = cross_term / (magnitude + (jnp.mean(magnitude) + EPSILON))
        full_corr = jnp.real(jnp.fft.ifftn(ratio_term)) * B ** 1.5
        idx_z = jnp.mod(column[5] + window_steps, B)
        idx_y = jnp.mod(column[6] + window_steps, B)
        idx_x = jnp.mod(column[7] + window_steps, B)
        values = full_corr[idx_z][:, idx_y][:, :, idx_x] * live_mask
        weight = values * values
        energy = jnp.mean(weight)
        steps_f = jnp.arange(WIN, dtype=jnp.float32)
        along_z = (column[5].astype(jnp.float32) + steps_f)[:, None, None]
        along_y = (column[6].astype(jnp.float32) + steps_f)[None, :, None]
        along_x = (column[7].astype(jnp.float32) + steps_f)[None, None, :]
        shift_vec = jnp.stack([jnp.mean(weight * along_z), jnp.mean(weight * along_y), jnp.mean(weight * along_x)]) / (energy + EPSILON)
        center = jnp.stack([
            (slab_pos.astype(jnp.float32) * B + 0.5 * B) / (B * N_SLAB),
            jnp.ones((), jnp.float32) * 0.5,
            (column[1].astype(jnp.float32) + 0.5 * B) / (2.0 * B),
            jnp.ones((), jnp.float32)])
        hit_a = (view_ids == column[0]).astype(jnp.float32)
        hit_b = (view_ids == column[2]).astype(jnp.float32)
        outer_hh = energy * center[:, None] * center[None, :]
        normal_part = (hit_a + hit_b)[:, None, None] * outer_hh[None]
        rhs_part = (hit_a - hit_b)[:, None, None] * (energy * center[:, None] * shift_vec[None, :])[None]
        return values.reshape(-1), shift_vec, normal_part, rhs_part

    corr_rows, shift_rows, normal_parts, rhs_parts = lax.map(one_pair, jnp.arange(pair_total, dtype=jnp.int32))
    normal_sums = jnp.sum(normal_parts, axis=0) / pair_total
    rhs_sums = jnp.sum(rhs_parts, axis=0) / pair_total
    return corr_rows, jnp.transpose(shift_rows), normal_sums, rhs_sums
```

```python
import functools

import jax
import jax.numpy as jnp
import numpy as np
from jax import lax
from jax.experimental import pallas as pl
from jax.experimental.pallas import tpu as pltpu
from jax.sharding import PartitionSpec as P

WIN = 8
NBR = 2
EPSILON = 1e-06
GAP = 8
PIECES = 4
PRECISE = lax.Precision.HIGHEST


def halves(table):
    table = table.astype(np.float32)
    high = table.astype(jnp.bfloat16)
    low = (table - high.astype(np.float32)).astype(jnp.bfloat16)
    return high, low


def three(table):
    high, low = halves(table)
    return np.concatenate([high, low, high], axis=1)


def padded(edge):
    return (edge // 2 + 1 + 7) // 8 * 8


def tiled(table):
    return np.ascontiguousarray(table.reshape(table.shape[0], -1, 128).transpose(1, 0, 2))


def static_tables(edge):
    half = edge // 2
    kept = padded(edge)
    ids = np.arange(edge)
    cells = np.arange(2 * edge) % edge
    angles = 2 * np.pi * (np.outer(cells, ids) % edge) / edge
    cos, sin, none = np.cos(angles), np.sin(angles), np.zeros((2 * edge, edge))
    table_x = np.concatenate(
        [
            np.concatenate([cos, none, -sin, none], axis=1),
            np.concatenate([none, cos, none, -sin], axis=1),
        ],
        axis=0,
    )
    table_x = np.concatenate(halves(table_x), axis=0).astype(np.float32)

    angles = 2 * np.pi * (np.outer(ids, ids) % edge) / edge
    cos, sin = np.cos(angles), np.sin(angles)
    table_z = three(np.block([[cos, sin], [-sin, cos]]))
    table_y = np.zeros((2 * kept, 2 * edge))
    table_y[: half + 1] = np.concatenate([cos, sin], axis=1)[: half + 1]
    table_y[kept : kept + half + 1] = np.concatenate([-sin, cos], axis=1)[: half + 1]
    table_y = three(table_y)

    steps = np.arange(edge + WIN) % edge
    angles = 2 * np.pi * (np.outer(steps, ids) % edge) / edge
    cos, sin = np.cos(angles), np.sin(angles)
    win_z = np.concatenate(
        [three(np.concatenate([cos, -sin], axis=1)), three(np.concatenate([sin, cos], axis=1))],
        axis=1,
    ).astype(np.float32)
    times = np.zeros((kept,))
    times[: half + 1] = 2.0
    times[0] = times[half] = 1.0
    cos_y = np.zeros((edge + WIN, kept))
    sin_y = np.zeros((edge + WIN, kept))
    cos_y[:, : half + 1] = cos[:, : half + 1]
    sin_y[:, : half + 1] = sin[:, : half + 1]
    cos_y, sin_y = cos_y * times, sin_y * times
    parts = []
    for part in ([cos_y, -sin_y], [sin_y, cos_y]):
        part = three(np.concatenate(part, axis=1)).astype(np.float32)
        extra = -part.shape[1] % 128
        parts.append(np.pad(part, ((0, 0), (0, extra))))
    win_y = np.concatenate(parts, axis=1)
    scale = edge**-1.5
    none = np.zeros_like(cos)
    win_x = np.concatenate(
        [cos * scale, none, -sin * scale, none, none, cos * scale, none, -sin * scale], axis=1
    ).astype(np.float32)
    return table_x, table_y, table_z, tiled(win_z), tiled(win_y), tiled(win_x)


def split(values):
    high = values.astype(jnp.bfloat16)
    return high, (values - high.astype(jnp.float32)).astype(jnp.bfloat16)


def fused_kernel(
    slab_count,
    fields_hbm,
    counts_hbm,
    volumes_hbm,
    tx_hbm,
    ty_hbm,
    tz_hbm,
    wz_hbm,
    wy_hbm,
    wx_hbm,
    corr_ref,
    shift_ref,
    sums_ref,
    fields_ref,
    counts_ref,
    held,
    tx,
    ty,
    tz,
    wz,
    wy,
    wx,
    request,
    asked,
    asked_smem,
    packed_first,
    packed_second,
    table_a,
    table_b,
    y_re,
    y_im,
    a_re,
    a_im,
    c_re,
    c_im,
    c_abs,
    g_re,
    g_im,
    part,
    parts,
    local_sems,
    load_sems,
    list_send,
    list_recv,
    send_sems,
    recv_sems,
    sum_send,
    sum_recv,
    *landed,
):
    edge = held.shape[1]
    lanes_all = 2 * edge
    half = edge // 2
    kept = padded(edge)
    pitch = edge + GAP
    cap = fields_ref.shape[1]
    views = held.shape[0]
    batches = cap // 2
    cells = half // PIECES
    own = lax.axis_index("slab")
    packed = (packed_first, packed_second)
    got = (landed[:PIECES], landed[PIECES:])

    small = [
        pltpu.make_async_copy(src, dst, local_sems.at[index])
        for index, (src, dst) in enumerate(
            (
                (fields_hbm, fields_ref),
                (counts_hbm, counts_ref),
                (tx_hbm, tx),
                (ty_hbm, ty),
                (tz_hbm, tz),
                (wz_hbm, wz),
                (wy_hbm, wy),
                (wx_hbm, wx),
            )
        )
    ]
    for copy in small:
        copy.start()
    step_z = edge // PIECES
    loads = [
        pltpu.make_async_copy(
            volumes_hbm.at[:, pl.ds(piece * step_z, step_z)],
            held.at[:, pl.ds(piece * step_z, step_z)],
            load_sems.at[piece],
        )
        for piece in range(PIECES)
    ]
    for copy in loads:
        copy.start()

    asked[...] = jnp.zeros_like(asked)
    present = (own > 0, own < slab_count - 1)
    peers = (lax.rem(own + slab_count - 1, slab_count), lax.rem(own + 1, slab_count))

    def on(side, action):
        pl.when(present[side])(action)

    barrier = pltpu.get_barrier_semaphore()

    def greet(step, _):
        pl.semaphore_signal(
            barrier,
            inc=1,
            device_id={"slab": lax.rem(own + step, slab_count)},
            device_id_type=pl.DeviceIdType.MESH,
        )
        return 0

    lax.fori_loop(1, slab_count, greet, 0)

    small[0].wait()
    small[1].wait()
    count = counts_ref[0]
    live = [count > slot for slot in range(cap)]
    direction = [jnp.where(live[slot], fields_ref[3, slot], 0) for slot in range(cap)]
    rank = []
    for slot in range(cap):
        seen = jnp.int32(0)
        for other in range(slot):
            seen = seen + (direction[other] == direction[slot]).astype(jnp.int32)
        rank.append(jnp.where(direction[slot] == 0, 0, seen))
    late = [(rank[slot] > 0).astype(jnp.int32) for slot in range(cap)]
    early_total = cap - sum(late)
    place = []
    early_seen, late_seen = jnp.int32(0), jnp.int32(0)
    for slot in range(cap):
        place.append(jnp.where(late[slot] > 0, early_total + late_seen, early_seen))
        early_seen = early_seen + 1 - late[slot]
        late_seen = late_seen + late[slot]

    def ordered(values):
        result = []
        for spot in range(cap):
            value = jnp.int32(0)
            for slot in range(cap):
                value = jnp.where(place[slot] == spot, values[slot], value)
            result.append(value)
        return result

    column = [
        ordered([jnp.where(live[slot], fields_ref[row, slot], 0) for slot in range(cap)])
        for row in range(8)
    ]
    slots = ordered([jnp.int32(slot) for slot in range(cap)])
    alive = ordered([live[slot].astype(jnp.int32) for slot in range(cap)])
    ranks = ordered(rank)

    lane8 = lax.broadcasted_iota(jnp.int32, request.shape[1:], 1)
    for side, wanted in enumerate((-1, 1)):
        values = jnp.zeros(request.shape[1:], jnp.int32)
        for level in range(NBR):
            view, anchor = jnp.int32(0), jnp.int32(0)
            for slot in range(cap):
                take = (direction[slot] == wanted) & (rank[slot] == level)
                view = jnp.where(take, fields_ref[2, slot], view)
                anchor = jnp.where(take, fields_ref[4, slot], anchor)
            values = jnp.where(lane8 == 2 * level, view, values)
            values = jnp.where(lane8 == 2 * level + 1, anchor, values)
        request[side] = values

    pl.semaphore_wait(barrier, slab_count - 1)

    def list_copy(side):
        return pltpu.make_async_remote_copy(
            src_ref=request.at[side],
            dst_ref=asked.at[1 - side],
            send_sem=list_send.at[side],
            recv_sem=list_recv.at[1 - side],
            device_id={"slab": peers[side]},
            device_id_type=pl.DeviceIdType.MESH,
        )

    def list_arrival(side):
        return pltpu.make_async_remote_copy(
            src_ref=request.at[side],
            dst_ref=asked.at[side],
            send_sem=list_send.at[side],
            recv_sem=list_recv.at[side],
            device_id={"slab": peers[side]},
            device_id_type=pl.DeviceIdType.MESH,
        )

    for side in range(2):
        on(side, lambda side=side: list_copy(side).start())

    for copy in small[2:]:
        copy.wait()
    rows = lax.broadcasted_iota(jnp.int32, (lanes_all, lanes_all), 0)

    def fill(table, starts):
        for piece in range(4):
            where = pl.ds(piece * lanes_all, lanes_all)
            start = starts[piece % 2]
            inside = (rows >= start) & (rows < start + edge)
            for side in range(2):
                cols = pl.ds(side * lanes_all, lanes_all)
                table[where, cols] = jnp.where(inside, tx[where, cols], 0.0).astype(jnp.bfloat16)

    for batch in range(batches):
        fill(table_a.at[batch], column[1][2 * batch : 2 * batch + 2])
        for part_z in range(2):
            fill(
                table_b.at[batch, part_z],
                [
                    jnp.where(column[3][spot] == 0, column[4][spot], part_z * edge)
                    for spot in range(2 * batch, 2 * batch + 2)
                ],
            )

    for side in range(2):
        on(side, lambda side=side: list_arrival(side).wait_recv())
    to_smem = pltpu.make_async_copy(asked, asked_smem, local_sems.at[0])
    to_smem.start()
    for copy in loads:
        copy.wait()
    to_smem.wait()

    def pack_piece(side, level, piece):
        view = asked_smem[side, 0, 2 * level]
        anchor = asked_smem[side, 0, 2 * level + 1]

        def step(index, _):
            z = piece * cells + index
            lanes = lax.broadcasted_iota(jnp.int32, (edge, lanes_all), 1)
            low = lanes < edge
            first = held[view, z].astype(jnp.float32)
            second = held[view, half + z].astype(jnp.float32)
            straight = jnp.where(low, first, second)
            turned = pltpu.roll(jnp.where(low, second, first), edge, 1)
            keep = (low & (lanes >= anchor)) | ((lanes >= edge) & (lanes < edge + anchor))
            packed[level][side, z] = jnp.where(keep, straight, turned).astype(jnp.bfloat16)
            return 0

        lax.fori_loop(0, cells, step, 0, unroll=True)

    def block_copy(side, level, piece):
        where = pl.ds(piece * cells, cells)
        return pltpu.make_async_remote_copy(
            src_ref=packed[level].at[side, where],
            dst_ref=got[level][piece].at[side],
            send_sem=send_sems.at[side, level, piece],
            recv_sem=recv_sems.at[side, level, piece],
            device_id={"slab": peers[side]},
            device_id_type=pl.DeviceIdType.MESH,
        )

    def block_arrival(side, level, piece):
        where = pl.ds(piece * cells, cells)
        return pltpu.make_async_remote_copy(
            src_ref=packed[level].at[side, where],
            dst_ref=got[level][piece].at[1 - side],
            send_sem=send_sems.at[side, level, piece],
            recv_sem=recv_sems.at[1 - side, level, piece],
            device_id={"slab": peers[side]},
            device_id_type=pl.DeviceIdType.MESH,
        )

    items = [
        (side, level, piece)
        for level in range(NBR)
        for piece in range(PIECES)
        for side in range(2)
    ]
    for number, item in enumerate(items):
        pack_piece(*item)
        if number:
            previous = items[number - 1]
            on(previous[0], lambda previous=previous: block_copy(*previous).start())
    on(items[-1][0], lambda: block_copy(*items[-1]).start())

    lanes = lax.broadcasted_iota(jnp.int32, (edge, lanes_all), 1)
    low = lanes < edge

    def xy_planes(left, right, table, z, planes):
        sides = jnp.concatenate(
            [
                left.reshape(planes * edge, lanes_all),
                right.reshape(planes * edge, lanes_all),
            ],
            axis=1,
        )
        mixed = jnp.dot(
            jnp.concatenate([sides, sides], axis=1), table, preferred_element_type=jnp.float32
        )
        high, rest = split(mixed)

        def planar(values, side):
            return jnp.concatenate(
                [
                    values[k * edge : (k + 1) * edge, side * lanes_all : (side + 1) * lanes_all]
                    for k in range(planes)
                ],
                axis=1,
            )

        highs = [planar(high, 0), planar(high, 1)]
        rests = [planar(rest, 0), planar(rest, 1)]
        mixed = jnp.dot(
            ty[...],
            jnp.concatenate(highs + highs + rests, axis=0),
            preferred_element_type=jnp.float32,
        )
        for index in range(planes):
            where = slice(index * lanes_all, (index + 1) * lanes_all)
            spots = pl.ds(z + index, half + 1, stride=pitch)
            y_re[spots, :] = mixed[: half + 1, where]
            y_im[spots, :] = mixed[kept : kept + half + 1, where]

    def z_plane(ky):
        where = pl.ds(pl.multiple_of(ky * pitch, 8), edge)
        real = split(y_re[where, :])
        imag = split(y_im[where, :])
        return [real[0], imag[0], real[0], imag[0], real[1], imag[1]]

    def z_planes(kys):
        stacks = [z_plane(ky) for ky in kys]
        mixed = jnp.dot(
            tz[...],
            jnp.concatenate(
                [jnp.concatenate([s[k] for s in stacks], axis=1) for k in range(6)], axis=0
            ),
            preferred_element_type=jnp.float32,
        )
        return [
            (
                mixed[:edge, k * lanes_all : (k + 1) * lanes_all],
                mixed[edge:, k * lanes_all : (k + 1) * lanes_all],
            )
            for k in range(len(kys))
        ]

    chunk = cells
    for batch in range(batches):
        views_a = column[0][2 * batch : 2 * batch + 2]

        def first_step(step, _, batch=batch, views_a=views_a):
            z = chunk * step
            xy_planes(
                held[views_a[0], pl.ds(z, chunk)],
                held[views_a[1], pl.ds(z, chunk)],
                table_a[batch],
                z,
                chunk,
            )
            return 0

        lax.fori_loop(0, edge // chunk, first_step, 0, unroll=2)

        def first_z(step, _, batch=batch):
            for ky, (real, imag) in zip(
                (2 * step, 2 * step + 1), z_planes((2 * step, 2 * step + 1))
            ):
                a_re[batch, ky] = real
                a_im[batch, ky] = imag
            return 0

        lax.fori_loop(0, half // 2, first_z, 0, unroll=4)
        ((real, imag),) = z_planes((half,))
        a_re[batch, half] = real
        a_im[batch, half] = imag

    g_re[pl.ds((half + 1) * WIN, (kept - half - 1) * WIN), :] = jnp.zeros(
        ((kept - half - 1) * WIN, lanes_all), jnp.float32
    )
    g_im[pl.ds((half + 1) * WIN, (kept - half - 1) * WIN), :] = jnp.zeros(
        ((kept - half - 1) * WIN, lanes_all), jnp.float32
    )

    total_cells = float(WIN**3)
    corr_all = jnp.zeros(corr_ref.shape, jnp.float32)
    shift_all = jnp.zeros(shift_ref.shape, jnp.float32)
    sums_all = jnp.zeros(part.shape, jnp.float32)

    for batch in range(batches):
        spots = (2 * batch, 2 * batch + 1)
        local = [column[3][spot] == 0 for spot in spots]
        which = [jnp.where(column[3][spot] < 0, 1, 0) for spot in spots]

        def second(q, piece, part_z, spots=spots, local=local, which=which, batch=batch):
            inner = held[column[2][spots[q]], pl.ds(part_z * half + piece * cells, cells)]
            outer = got[0][piece][which[q]]
            if batch:
                outer = jnp.where(ranks[spots[q]] > 0, got[1][piece][which[q]], outer)
            return jnp.where(local[q], inner, outer)

        for piece in range(PIECES):
            for side in range(2):
                on(
                    side,
                    lambda side=side, piece=piece: block_arrival(side, batch, piece).wait_recv(),
                )
            for part_z in range(2):
                xy_planes(
                    second(0, piece, part_z),
                    second(1, piece, part_z),
                    table_b[batch, part_z],
                    part_z * half + piece * cells,
                    cells,
                )

        def cross_plane(ky, real, imag, total, times, batch=batch):
            front_re, front_im = a_re[batch, ky], a_im[batch, ky]
            cross_re = front_re * real + front_im * imag
            cross_im = front_im * real - front_re * imag
            size = jnp.sqrt(cross_re * cross_re + cross_im * cross_im)
            c_re[ky] = cross_re
            c_im[ky] = cross_im
            c_abs[ky] = size
            return total + times * size

        def second_z(step, total, batch=batch):
            kys = (2 * step, 2 * step + 1)
            for ky, (real, imag) in zip(kys, z_planes(kys)):
                total = cross_plane(ky, real, imag, total, jnp.where(ky == 0, 1.0, 2.0))
            return total

        total = lax.fori_loop(
            0, half // 2, second_z, jnp.zeros((edge, lanes_all), jnp.float32), unroll=4
        )
        ((real, imag),) = z_planes((half,))
        total = cross_plane(half, real, imag, total, 1.0)
        floors = [
            jnp.sum(jnp.where(mask, total, 0.0)) / float(edge**3) + EPSILON
            for mask in (low, jnp.logical_not(low))
        ]
        floor = jnp.where(low, floors[0], floors[1])

        def row_of(value):
            return lax.rem(value + 4 * edge, edge)

        def window_rows(ref, start, first, last):
            return jnp.concatenate(
                [ref[k, pl.ds(start, WIN), :] for k in range(first, last)], axis=1
            )

        wide = wz.shape[0] // 2
        starts = [row_of(column[5][spot]) for spot in spots]
        table_w = jnp.concatenate(
            [
                window_rows(wz, starts[q], kind * wide, (kind + 1) * wide)
                for q in range(2)
                for kind in range(2)
            ],
            axis=0,
        ).astype(jnp.bfloat16)
        low_w = low[:WIN]

        def window_planes(kys, floor=floor, table_w=table_w):
            stacks = []
            for ky in kys:
                inverse = 1.0 / (c_abs[ky] + floor)
                real = split(c_re[ky] * inverse)
                imag = split(c_im[ky] * inverse)
                stacks.append([real[0], imag[0], real[0], imag[0], real[1], imag[1]])
            mixed = jnp.dot(
                table_w,
                jnp.concatenate(
                    [jnp.concatenate([s[k] for s in stacks], axis=1) for k in range(6)], axis=0
                ),
                preferred_element_type=jnp.float32,
            )
            for k, ky in enumerate(kys):
                cut = mixed[:, k * lanes_all : (k + 1) * lanes_all]
                where = pl.ds(pl.multiple_of(ky * WIN, 8), WIN)
                g_re[where, :] = jnp.where(low_w, cut[:WIN], cut[2 * WIN : 3 * WIN])
                g_im[where, :] = jnp.where(low_w, cut[WIN : 2 * WIN], cut[3 * WIN :])

        def window_step(step, _):
            window_planes((2 * step, 2 * step + 1))
            return 0

        lax.fori_loop(0, half // 2, window_step, 0, unroll=4)
        window_planes((half,))

        stack = jnp.concatenate(
            [
                jnp.concatenate(
                    [ref[pl.ds(i, kept, stride=WIN), :] for i in range(WIN)], axis=1
                )
                for ref in (g_re, g_im)
            ],
            axis=0,
        )
        high, rest = split(stack)
        deep = 6 * kept
        wide = wy.shape[0] // 2
        starts = [row_of(column[6][spot]) for spot in spots]
        table_w = jnp.concatenate(
            [
                window_rows(wy, starts[q], kind * wide, (kind + 1) * wide)
                for q in range(2)
                for kind in range(2)
            ],
            axis=0,
        ).astype(jnp.bfloat16)[:, :deep]
        mixed = jnp.dot(
            table_w,
            jnp.concatenate([high, high, rest], axis=0),
            preferred_element_type=jnp.float32,
        )
        fronts = []
        for kind in range(2):
            pieces = []
            for i in range(WIN):
                where = slice(i * lanes_all, (i + 1) * lanes_all)
                pieces.append(
                    jnp.where(
                        low_w,
                        mixed[kind * WIN : (kind + 1) * WIN, where],
                        mixed[(2 + kind) * WIN : (3 + kind) * WIN, where],
                    )
                )
            fronts.append(jnp.concatenate(pieces, axis=0))
        starts = [row_of(column[7][spot] + column[1][spot] - column[4][spot]) for spot in spots]
        table_w = jnp.concatenate(
            [
                window_rows(wx, starts[q], q * (wx.shape[0] // 2), (q + 1) * (wx.shape[0] // 2))
                for q in range(2)
            ],
            axis=0,
        )
        values = lax.dot_general(
            jnp.concatenate(fronts, axis=1),
            table_w,
            (((1,), (1,)), ((), ())),
            precision=PRECISE,
            preferred_element_type=jnp.float32,
        )
        line = lax.broadcasted_iota(jnp.int32, values.shape, 0)
        lane = lax.broadcasted_iota(jnp.int32, values.shape, 1)
        low_v = lane < WIN
        values = values * jnp.where(
            low_v, alive[spots[0]].astype(jnp.float32), alive[spots[1]].astype(jnp.float32)
        )
        weight = values * values
        places = (line // WIN, line % WIN, lane % WIN)
        long = corr_ref.shape[1]
        place_row = lax.broadcasted_iota(jnp.int32, (2 * WIN, long), 0)
        place_lane = lax.broadcasted_iota(jnp.int32, (2 * WIN, long), 1)
        spread_row = lax.broadcasted_iota(jnp.int32, (WIN * WIN, long), 0)
        spread_lane = lax.broadcasted_iota(jnp.int32, (WIN * WIN, long), 1)
        for q, spot in enumerate(spots):
            mask = low_v if q == 0 else jnp.logical_not(low_v)
            mine = jnp.where(mask, weight, 0.0)
            energy = jnp.sum(mine, keepdims=True) / total_cells
            shifts = [
                (
                    jnp.sum(mine * where.astype(jnp.float32), keepdims=True) / total_cells
                    + energy * column[5 + axis][spot].astype(jnp.float32)
                )
                / (energy + EPSILON)
                for axis, where in enumerate(places)
            ]
            pick = (place_row == place_lane % WIN + q * WIN).astype(jnp.float32)
            spread = jnp.dot(
                values, pick, precision=PRECISE, preferred_element_type=jnp.float32
            )
            line_out = jnp.sum(
                jnp.where(spread_lane // WIN == spread_row, spread, 0.0), axis=0, keepdims=True
            )
            slot_row = lax.broadcasted_iota(jnp.int32, corr_ref.shape, 0)
            corr_all = jnp.where(slot_row == slots[spot], line_out, corr_all)

            spot_row = lax.broadcasted_iota(jnp.int32, shift_ref.shape, 0)
            spot_lane = lax.broadcasted_iota(jnp.int32, shift_ref.shape, 1)
            for axis in range(3):
                shift_all = jnp.where(
                    (spot_row == axis) & (spot_lane == slots[spot]), shifts[axis], shift_all
                )

            view = lax.broadcasted_iota(jnp.int32, part.shape, 0)
            entry = lax.broadcasted_iota(jnp.int32, part.shape, 1)
            center_z = (own.astype(jnp.float32) * edge + 0.5 * edge) / float(edge * slab_count)
            center_x = (column[1][spot].astype(jnp.float32) + 0.5 * edge) / (2.0 * edge)

            def center(index, center_z=center_z, center_x=center_x):
                return jnp.where(
                    index == 0,
                    center_z,
                    jnp.where(index == 1, 0.5, jnp.where(index == 2, center_x, 1.0)),
                )

            hit_a = (view == column[0][spot]).astype(jnp.float32)
            hit_b = (view == column[2][spot]).astype(jnp.float32)
            normal = (hit_a + hit_b) * center(entry // 4) * center(entry % 4)
            after = jnp.maximum(entry - 16, 0)
            third = after % 3
            shift = jnp.where(third == 0, shifts[0], jnp.where(third == 1, shifts[1], shifts[2]))
            rhs = (hit_a - hit_b) * center(after // 3) * shift
            sums_all = sums_all + jnp.where(
                entry < 16, normal, jnp.where(entry < 28, rhs, 0.0)
            ) * (energy / float(cap * slab_count))

    part[...] = sums_all
    corr_ref[...] = corr_all
    shift_ref[...] = shift_all

    def part_copy(peer, source):
        return pltpu.make_async_remote_copy(
            src_ref=part,
            dst_ref=parts.at[source],
            send_sem=sum_send.at[peer],
            recv_sem=sum_recv.at[source],
            device_id={"slab": peer},
            device_id_type=pl.DeviceIdType.MESH,
        )

    def send_part(step, _):
        part_copy(lax.rem(own + step, slab_count), own).start()
        return 0

    lax.fori_loop(1, slab_count, send_part, 0)
    parts[own] = part[...]
    for side in range(2):
        on(side, lambda side=side: list_copy(side).wait_send())
    for item in items:
        on(item[0], lambda item=item: block_copy(*item).wait_send())

    def wait_part(step, _):
        peer = lax.rem(own + step, slab_count)
        part_copy(peer, own).wait_send()
        part_copy(peer, peer).wait_recv()
        return 0

    lax.fori_loop(1, slab_count, wait_part, 0)
    sums_ref[...] = lax.fori_loop(
        1, slab_count, lambda index, total: total + parts[index], parts[0]
    )


def fused(volumes, pair_fields, pair_counts, slab_count):
    views, edge = volumes.shape[0], volumes.shape[1]
    cap = pair_fields.shape[1]
    lanes = 2 * edge
    half = edge // 2
    kept = padded(edge)
    tables = static_tables(edge)
    vmem = pl.BlockSpec(memory_space=pltpu.VMEM)
    hbm = pl.BlockSpec(memory_space=pltpu.HBM)
    f32, bf16 = jnp.float32, jnp.bfloat16
    spectrum = (half + 1, edge, lanes)
    return pl.pallas_call(
        functools.partial(fused_kernel, slab_count),
        out_shape=(
            jax.ShapeDtypeStruct((cap, WIN**3), f32),
            jax.ShapeDtypeStruct((8, lanes), f32),
            jax.ShapeDtypeStruct((views, lanes), f32),
        ),
        in_specs=[hbm] * (3 + len(tables)),
        out_specs=(vmem, vmem, vmem),
        scratch_shapes=[
            pltpu.SMEM(pair_fields.shape, jnp.int32),
            pltpu.SMEM(pair_counts.shape, jnp.int32),
            pltpu.VMEM(volumes.shape, bf16),
        ]
        + [pltpu.VMEM(table.shape, table.dtype) for table in tables]
        + [
            pltpu.VMEM((2, 8, lanes), jnp.int32),
            pltpu.VMEM((2, 8, lanes), jnp.int32),
            pltpu.SMEM((2, 8, lanes), jnp.int32),
            pltpu.VMEM((2, half, edge, lanes), bf16),
            pltpu.VMEM((2, half, edge, lanes), bf16),
            pltpu.VMEM((cap // 2, 4 * lanes, 2 * lanes), bf16),
            pltpu.VMEM((cap // 2, 2, 4 * lanes, 2 * lanes), bf16),
            pltpu.VMEM((kept * (edge + GAP), lanes), f32),
            pltpu.VMEM((kept * (edge + GAP), lanes), f32),
            pltpu.VMEM((cap // 2,) + spectrum, f32),
            pltpu.VMEM((cap // 2,) + spectrum, f32),
            pltpu.VMEM(spectrum, f32),
            pltpu.VMEM(spectrum, f32),
            pltpu.VMEM(spectrum, f32),
            pltpu.VMEM((kept * WIN, lanes), f32),
            pltpu.VMEM((kept * WIN, lanes), f32),
            pltpu.VMEM((views, lanes), f32),
            pltpu.VMEM((slab_count, views, lanes), f32),
            pltpu.SemaphoreType.DMA((2 + len(tables),)),
            pltpu.SemaphoreType.DMA((PIECES,)),
            pltpu.SemaphoreType.DMA((2,)),
            pltpu.SemaphoreType.DMA((2,)),
            pltpu.SemaphoreType.DMA((2, NBR, PIECES)),
            pltpu.SemaphoreType.DMA((2, NBR, PIECES)),
            pltpu.SemaphoreType.DMA((slab_count,)),
            pltpu.SemaphoreType.DMA((slab_count,)),
        ]
        + [pltpu.VMEM((2, half // PIECES, edge, lanes), bf16)] * (NBR * PIECES),
        compiler_params=pltpu.CompilerParams(
            collective_id=1, has_side_effects=True, vmem_limit_bytes=60 * 2**20
        ),
        name="fused",
    )(pair_fields, pair_counts, volumes, *[jnp.asarray(table) for table in tables])


def on_device(volumes, pair_fields, pair_counts):
    cap = pair_fields.shape[1]
    slab_count = lax.axis_size("slab")
    corr, shifts, sums = fused(volumes, pair_fields, pair_counts, slab_count)
    return (
        corr,
        shifts[:3, :cap],
        sums[:, :16].reshape(-1, 4, 4),
        sums[:, 16:28].reshape(-1, 4, 3),
    )


def solution(mesh):
    in_specs = (P("tm", "slab", None, None), P(None, ("tm", "slab")), P(("tm", "slab")))
    out_specs = (
        P(("tm", "slab"), None),
        P(None, ("tm", "slab")),
        P("tm", None, None),
        P("tm", None, None),
    )
    return jax.shard_map(
        on_device, mesh=mesh, in_specs=in_specs, out_specs=out_specs, check_vma=False
    )
```

```python
import functools

import jax
import jax.numpy as jnp
import numpy as np
from jax import lax
from jax.experimental import pallas as pl
from jax.experimental.pallas import tpu as pltpu
from jax.sharding import PartitionSpec as P

WIN = 8
NBR = 2
EPSILON = 1e-06
GAP = 4
PIECES = 4
PRECISE = lax.Precision.HIGHEST


def halves(table):
    table = table.astype(np.float32)
    high = table.astype(jnp.bfloat16)
    low = (table - high.astype(np.float32)).astype(jnp.bfloat16)
    return high, low


def three(table):
    high, low = halves(table)
    return np.concatenate([high, low, high], axis=1)


def padded(edge):
    return (edge // 2 + 1 + 7) // 8 * 8


def tiled(table):
    return np.ascontiguousarray(table.reshape(table.shape[0], -1, 128).transpose(1, 0, 2))


def static_tables(edge):
    half = edge // 2
    kept = padded(edge)
    ids = np.arange(edge)
    cells = np.arange(2 * edge) % edge
    angles = 2 * np.pi * (np.outer(cells, ids) % edge) / edge
    cos, sin, none = np.cos(angles), np.sin(angles), np.zeros((2 * edge, edge))
    table_x = np.concatenate(
        [
            np.concatenate([cos, none, -sin, none], axis=1),
            np.concatenate([none, cos, none, -sin], axis=1),
        ],
        axis=0,
    )
    table_x = np.concatenate(halves(table_x), axis=0).astype(np.float32)

    angles = 2 * np.pi * (np.outer(ids, ids) % edge) / edge
    cos, sin = np.cos(angles), np.sin(angles)
    table_z = three(np.block([[cos, sin], [-sin, cos]]))
    table_y = np.zeros((2 * kept, 2 * edge))
    table_y[: half + 1] = np.concatenate([cos, sin], axis=1)[: half + 1]
    table_y[kept : kept + half + 1] = np.concatenate([-sin, cos], axis=1)[: half + 1]
    table_y = three(table_y)

    steps = np.arange(edge + WIN) % edge
    angles = 2 * np.pi * (np.outer(steps, ids) % edge) / edge
    cos, sin = np.cos(angles), np.sin(angles)
    win_z = np.concatenate(
        [three(np.concatenate([cos, -sin], axis=1)), three(np.concatenate([sin, cos], axis=1))],
        axis=1,
    ).astype(np.float32)
    times = np.zeros((kept,))
    times[: half + 1] = 2.0
    times[0] = times[half] = 1.0
    cos_y = np.zeros((edge + WIN, kept))
    sin_y = np.zeros((edge + WIN, kept))
    cos_y[:, : half + 1] = cos[:, : half + 1]
    sin_y[:, : half + 1] = sin[:, : half + 1]
    cos_y, sin_y = cos_y * times, sin_y * times
    parts = []
    for part in ([cos_y, -sin_y], [sin_y, cos_y]):
        part = three(np.concatenate(part, axis=1)).astype(np.float32)
        extra = -part.shape[1] % 128
        parts.append(np.pad(part, ((0, 0), (0, extra))))
    win_y = np.concatenate(parts, axis=1)
    scale = edge**-1.5
    none = np.zeros_like(cos)
    win_x = np.concatenate(
        [cos * scale, none, -sin * scale, none, none, cos * scale, none, -sin * scale], axis=1
    ).astype(np.float32)
    return table_x, table_y, table_z, tiled(win_z), tiled(win_y), tiled(win_x)


def split(values):
    high = values.astype(jnp.bfloat16)
    return high, (values - high.astype(jnp.float32)).astype(jnp.bfloat16)


def fused_kernel(
    slab_count,
    fields_hbm,
    counts_hbm,
    volumes_hbm,
    tx_hbm,
    ty_hbm,
    tz_hbm,
    wz_hbm,
    wy_hbm,
    wx_hbm,
    corr_ref,
    shift_ref,
    sums_ref,
    fields_ref,
    counts_ref,
    held,
    tx,
    ty,
    tz,
    wz,
    wy,
    wx,
    request,
    asked,
    packed_first,
    packed_second,
    table_a,
    table_b,
    x_high,
    x_rest,
    y_re,
    y_im,
    a_re,
    a_im,
    c_re,
    c_im,
    c_abs,
    g_re,
    g_im,
    part,
    parts,
    local_sems,
    load_sems,
    list_send,
    list_recv,
    send_sems,
    recv_sems,
    sum_send,
    sum_recv,
    *landed,
):
    edge = held.shape[1]
    lanes_all = 2 * edge
    half = edge // 2
    kept = padded(edge)
    pitch = edge + GAP
    cap = fields_ref.shape[0]
    views = held.shape[0]
    batches = cap // 2
    cells = half // PIECES
    own = lax.axis_index("slab")
    packed = (packed_first, packed_second)
    got = (landed[:PIECES], landed[PIECES:])

    small = [
        pltpu.make_async_copy(src, dst, local_sems.at[index])
        for index, (src, dst) in enumerate(
            (
                (fields_hbm, fields_ref),
                (counts_hbm, counts_ref),
                (tx_hbm, tx),
                (ty_hbm, ty),
                (tz_hbm, tz),
                (wz_hbm, wz),
                (wy_hbm, wy),
                (wx_hbm, wx),
            )
        )
    ]
    for copy in small:
        copy.start()
    step_z = edge // PIECES
    loads = [
        pltpu.make_async_copy(
            volumes_hbm.at[:, pl.ds(piece * step_z, step_z)],
            held.at[:, pl.ds(piece * step_z, step_z)],
            load_sems.at[piece],
        )
        for piece in range(PIECES)
    ]
    for copy in loads:
        copy.start()

    for side in range(2):
        for index in range(2 * NBR):
            asked[side, 0, index] = 0
    present = (own > 0, own < slab_count - 1)
    peers = (lax.rem(own + slab_count - 1, slab_count), lax.rem(own + 1, slab_count))

    def on(side, action):
        pl.when(present[side])(action)

    barrier = pltpu.get_barrier_semaphore()

    def greet(step, _):
        pl.semaphore_signal(
            barrier,
            inc=1,
            device_id={"slab": lax.rem(own + step, slab_count)},
            device_id_type=pl.DeviceIdType.MESH,
        )
        return 0

    lax.fori_loop(1, slab_count, greet, 0)

    small[0].wait()
    small[1].wait()
    count = counts_ref[0]
    live = [count > slot for slot in range(cap)]
    direction = [jnp.where(live[slot], fields_ref[slot, 3], 0) for slot in range(cap)]
    rank = []
    for slot in range(cap):
        seen = jnp.int32(0)
        for other in range(slot):
            seen = seen + (direction[other] == direction[slot]).astype(jnp.int32)
        rank.append(jnp.where(direction[slot] == 0, 0, seen))
    late = [(rank[slot] > 0).astype(jnp.int32) for slot in range(cap)]
    early_total = cap - sum(late)
    place = []
    early_seen, late_seen = jnp.int32(0), jnp.int32(0)
    for slot in range(cap):
        place.append(jnp.where(late[slot] > 0, early_total + late_seen, early_seen))
        early_seen = early_seen + 1 - late[slot]
        late_seen = late_seen + late[slot]

    def ordered(values):
        result = []
        for spot in range(cap):
            value = jnp.int32(0)
            for slot in range(cap):
                value = jnp.where(place[slot] == spot, values[slot], value)
            result.append(value)
        return result

    column = [
        ordered([jnp.where(live[slot], fields_ref[slot, row], 0) for slot in range(cap)])
        for row in range(8)
    ]
    slots = ordered([jnp.int32(slot) for slot in range(cap)])
    alive = ordered([live[slot].astype(jnp.int32) for slot in range(cap)])
    ranks = ordered(rank)

    lane8 = lax.broadcasted_iota(jnp.int32, request.shape[1:], 1)
    for side, wanted in enumerate((-1, 1)):
        values = jnp.zeros(request.shape[1:], jnp.int32)
        for level in range(NBR):
            view, anchor = jnp.int32(0), jnp.int32(0)
            for slot in range(cap):
                take = (direction[slot] == wanted) & (rank[slot] == level)
                view = jnp.where(take, fields_ref[slot, 2], view)
                anchor = jnp.where(take, fields_ref[slot, 4], anchor)
            values = jnp.where(lane8 == 2 * level, view, values)
            values = jnp.where(lane8 == 2 * level + 1, anchor, values)
        request[side] = values

    pl.semaphore_wait(barrier, slab_count - 1)

    def list_copy(side):
        return pltpu.make_async_remote_copy(
            src_ref=request.at[side],
            dst_ref=asked.at[1 - side],
            send_sem=list_send.at[side],
            recv_sem=list_recv.at[1 - side],
            device_id={"slab": peers[side]},
            device_id_type=pl.DeviceIdType.MESH,
        )

    def list_arrival(side):
        return pltpu.make_async_remote_copy(
            src_ref=request.at[side],
            dst_ref=asked.at[side],
            send_sem=list_send.at[side],
            recv_sem=list_recv.at[side],
            device_id={"slab": peers[side]},
            device_id_type=pl.DeviceIdType.MESH,
        )

    for side in range(2):
        on(side, lambda side=side: list_copy(side).start())

    for copy in small[2:]:
        copy.wait()
    rows = lax.broadcasted_iota(jnp.int32, (lanes_all, lanes_all), 0)

    def fill(table, starts):
        for piece in range(4):
            where = pl.ds(piece * lanes_all, lanes_all)
            start = starts[piece % 2]
            inside = (rows >= start) & (rows < start + edge)
            for side in range(2):
                cols = pl.ds(side * lanes_all, lanes_all)
                table[where, cols] = jnp.where(inside, tx[where, cols], 0.0).astype(jnp.bfloat16)

    for batch in range(batches):
        fill(table_a.at[batch], column[1][2 * batch : 2 * batch + 2])
        for part_z in range(2):
            fill(
                table_b.at[batch, part_z],
                [
                    jnp.where(column[3][spot] == 0, column[4][spot], part_z * edge)
                    for spot in range(2 * batch, 2 * batch + 2)
                ],
            )

    for side in range(2):
        on(side, lambda side=side: list_arrival(side).wait_recv())
    for copy in loads:
        copy.wait()

    def pack_piece(side, level, piece):
        view = asked[side, 0, 2 * level]
        anchor = asked[side, 0, 2 * level + 1]

        def step(index, _):
            z = piece * cells + index
            lanes = lax.broadcasted_iota(jnp.int32, (edge, lanes_all), 1)
            low = lanes < edge
            first = held[view, z].astype(jnp.float32)
            second = held[view, half + z].astype(jnp.float32)
            straight = jnp.where(low, first, second)
            turned = pltpu.roll(jnp.where(low, second, first), edge, 1)
            keep = (low & (lanes >= anchor)) | ((lanes >= edge) & (lanes < edge + anchor))
            packed[level][side, z] = jnp.where(keep, straight, turned).astype(jnp.bfloat16)
            return 0

        lax.fori_loop(0, cells, step, 0, unroll=True)

    def block_copy(side, level, piece):
        where = pl.ds(piece * cells, cells)
        return pltpu.make_async_remote_copy(
            src_ref=packed[level].at[side, where],
            dst_ref=got[level][piece].at[side],
            send_sem=send_sems.at[side, level, piece],
            recv_sem=recv_sems.at[side, level, piece],
            device_id={"slab": peers[side]},
            device_id_type=pl.DeviceIdType.MESH,
        )

    def block_arrival(side, level, piece):
        where = pl.ds(piece * cells, cells)
        return pltpu.make_async_remote_copy(
            src_ref=packed[level].at[side, where],
            dst_ref=got[level][piece].at[1 - side],
            send_sem=send_sems.at[side, level, piece],
            recv_sem=recv_sems.at[1 - side, level, piece],
            device_id={"slab": peers[side]},
            device_id_type=pl.DeviceIdType.MESH,
        )

    items = [
        (side, level, piece)
        for level in range(NBR)
        for piece in range(PIECES)
        for side in range(2)
    ]
    turn = lax.rem(own, 4)
    odd = (turn == 0, turn == 3)

    def send_later(moment):
        for item in items:
            if item[1] > 0:
                mine = odd[item[0]] if moment else jnp.logical_not(odd[item[0]])
                pl.when(present[item[0]] & mine)(lambda item=item: block_copy(*item).start())

    def pack_level(level, send):
        mine = [item for item in items if item[1] == level]
        for number, item in enumerate(mine):
            pack_piece(*item)
            if number and send:
                previous = mine[number - 1]
                on(previous[0], lambda previous=previous: block_copy(*previous).start())
        if send:
            on(mine[-1][0], lambda: block_copy(*mine[-1]).start())

    pack_level(0, True)

    lanes = lax.broadcasted_iota(jnp.int32, (edge, lanes_all), 1)
    low = lanes < edge

    def x_planes(left, right, table, z, planes):
        sides = jnp.concatenate(
            [
                left.reshape(planes * edge, lanes_all),
                right.reshape(planes * edge, lanes_all),
            ],
            axis=1,
        )
        mixed = jnp.dot(
            jnp.concatenate([sides, sides], axis=1), table, preferred_element_type=jnp.float32
        )
        high, rest = split(mixed)
        where = pl.ds(z * edge, planes * edge)
        for side in range(2):
            cols = slice(side * lanes_all, (side + 1) * lanes_all)
            x_high[side, where, :] = high[:, cols]
            x_rest[side, where, :] = rest[:, cols]

    def y_planes(z, planes):
        def planar(ref, side):
            return jnp.concatenate(
                [ref[side, pl.ds((z + k) * edge, edge), :] for k in range(planes)], axis=1
            )

        highs = [planar(x_high, 0), planar(x_high, 1)]
        rests = [planar(x_rest, 0), planar(x_rest, 1)]
        mixed = jnp.dot(
            ty[...],
            jnp.concatenate(highs + highs + rests, axis=0),
            preferred_element_type=jnp.float32,
        )
        for index in range(planes):
            where = slice(index * lanes_all, (index + 1) * lanes_all)
            spots = pl.ds(z + index, half + 1, stride=pitch)
            y_re[spots, :] = mixed[: half + 1, where]
            y_im[spots, :] = mixed[kept : kept + half + 1, where]

    def z_plane(ky):
        where = pl.ds(ky * pitch, edge)
        real = split(y_re[where, :])
        imag = split(y_im[where, :])
        return [real[0], imag[0], real[0], imag[0], real[1], imag[1]]

    def z_planes(kys):
        stacks = [z_plane(ky) for ky in kys]
        mixed = jnp.dot(
            tz[...],
            jnp.concatenate(
                [jnp.concatenate([s[k] for s in stacks], axis=1) for k in range(6)], axis=0
            ),
            preferred_element_type=jnp.float32,
        )
        return [
            (
                mixed[:edge, k * lanes_all : (k + 1) * lanes_all],
                mixed[edge:, k * lanes_all : (k + 1) * lanes_all],
            )
            for k in range(len(kys))
        ]

    chunk = edge // 4
    for batch in range(batches):
        views_a = column[0][2 * batch : 2 * batch + 2]

        def first_x(step, batch=batch, views_a=views_a):
            z = chunk * step
            x_planes(
                held[views_a[0], pl.ds(z, chunk)],
                held[views_a[1], pl.ds(z, chunk)],
                table_a[batch],
                z,
                chunk,
            )

        def first_step(step, _, first_x=first_x):
            y_planes(chunk * step, chunk)
            first_x(step + 1)
            return 0

        first_x(0)
        lax.fori_loop(0, edge // chunk - 1, first_step, 0)
        y_planes(edge - chunk, chunk)

        def first_z(step, _, batch=batch):
            for ky, (real, imag) in zip(
                (2 * step, 2 * step + 1), z_planes((2 * step, 2 * step + 1))
            ):
                a_re[batch, ky] = real
                a_im[batch, ky] = imag
            return 0

        lax.fori_loop(0, half // 2, first_z, 0, unroll=4)
        ((real, imag),) = z_planes((half,))
        a_re[batch, half] = real
        a_im[batch, half] = imag
        if batch == 0:
            for level in range(1, NBR):
                pack_level(level, False)

    send_later(0)

    g_re[pl.ds((half + 1) * WIN, (kept - half - 1) * WIN), :] = jnp.zeros(
        ((kept - half - 1) * WIN, lanes_all), jnp.float32
    )
    g_im[pl.ds((half + 1) * WIN, (kept - half - 1) * WIN), :] = jnp.zeros(
        ((kept - half - 1) * WIN, lanes_all), jnp.float32
    )

    total_cells = float(WIN**3)
    corr_all = jnp.zeros(corr_ref.shape, jnp.float32)
    shift_all = jnp.zeros(shift_ref.shape, jnp.float32)
    sums_all = jnp.zeros(part.shape, jnp.float32)

    for batch in range(batches):
        spots = (2 * batch, 2 * batch + 1)
        local = [column[3][spot] == 0 for spot in spots]
        which = [jnp.where(column[3][spot] < 0, 1, 0) for spot in spots]

        def second(q, piece, part_z, spots=spots, local=local, which=which, batch=batch):
            inner = held[column[2][spots[q]], pl.ds(part_z * half + piece * cells, cells)]
            outer = got[0][piece][which[q]]
            if batch:
                outer = jnp.where(ranks[spots[q]] > 0, got[1][piece][which[q]], outer)
            return jnp.where(local[q], inner, outer)

        for piece in range(PIECES):
            for side in range(2):
                on(
                    side,
                    lambda side=side, piece=piece: block_arrival(side, batch, piece).wait_recv(),
                )
            for part_z in range(2):
                x_planes(
                    second(0, piece, part_z),
                    second(1, piece, part_z),
                    table_b[batch, part_z],
                    part_z * half + piece * cells,
                    cells,
                )
            for part_z in range(2):
                if piece:
                    y_planes(part_z * half + (piece - 1) * cells, cells)
            if batch == 0 and piece == PIECES // 2:
                send_later(1)
        for part_z in range(2):
            y_planes(part_z * half + (PIECES - 1) * cells, cells)

        def cross_plane(ky, real, imag, total, times, batch=batch):
            front_re, front_im = a_re[batch, ky], a_im[batch, ky]
            cross_re = front_re * real + front_im * imag
            cross_im = front_im * real - front_re * imag
            size = jnp.sqrt(cross_re * cross_re + cross_im * cross_im)
            c_re[ky] = cross_re
            c_im[ky] = cross_im
            c_abs[ky] = size
            return total + times * size

        def second_z(step, total, batch=batch):
            kys = (2 * step, 2 * step + 1)
            for ky, (real, imag) in zip(kys, z_planes(kys)):
                total = cross_plane(ky, real, imag, total, jnp.where(ky == 0, 1.0, 2.0))
            return total

        total = lax.fori_loop(
            0, half // 2, second_z, jnp.zeros((edge, lanes_all), jnp.float32), unroll=4
        )
        ((real, imag),) = z_planes((half,))
        total = cross_plane(half, real, imag, total, 1.0)
        floors = [
            jnp.sum(jnp.where(mask, total, 0.0)) / float(edge**3) + EPSILON
            for mask in (low, jnp.logical_not(low))
        ]
        floor = jnp.where(low, floors[0], floors[1])

        def row_of(value):
            return lax.rem(value + 4 * edge, edge)

        def window_rows(ref, start, first, last):
            return jnp.concatenate(
                [ref[k, pl.ds(start, WIN), :] for k in range(first, last)], axis=1
            )

        wide = wz.shape[0] // 2
        starts = [row_of(column[5][spot]) for spot in spots]
        table_w = jnp.concatenate(
            [
                window_rows(wz, starts[q], kind * wide, (kind + 1) * wide)
                for q in range(2)
                for kind in range(2)
            ],
            axis=0,
        ).astype(jnp.bfloat16)
        low_w = low[:WIN]

        def window_planes(kys, floor=floor, table_w=table_w):
            stacks = []
            for ky in kys:
                inverse = 1.0 / (c_abs[ky] + floor)
                real = split(c_re[ky] * inverse)
                imag = split(c_im[ky] * inverse)
                stacks.append([real[0], imag[0], real[0], imag[0], real[1], imag[1]])
            mixed = jnp.dot(
                table_w,
                jnp.concatenate(
                    [jnp.concatenate([s[k] for s in stacks], axis=1) for k in range(6)], axis=0
                ),
                preferred_element_type=jnp.float32,
            )
            for k, ky in enumerate(kys):
                cut = mixed[:, k * lanes_all : (k + 1) * lanes_all]
                where = pl.ds(pl.multiple_of(ky * WIN, 8), WIN)
                g_re[where, :] = jnp.where(low_w, cut[:WIN], cut[2 * WIN : 3 * WIN])
                g_im[where, :] = jnp.where(low_w, cut[WIN : 2 * WIN], cut[3 * WIN :])

        def window_step(step, _):
            window_planes((2 * step, 2 * step + 1))
            return 0

        lax.fori_loop(0, half // 2, window_step, 0, unroll=4)
        window_planes((half,))

        stack = jnp.concatenate(
            [
                jnp.concatenate(
                    [ref[pl.ds(i, kept, stride=WIN), :] for i in range(WIN)], axis=1
                )
                for ref in (g_re, g_im)
            ],
            axis=0,
        )
        high, rest = split(stack)
        deep = 6 * kept
        wide = wy.shape[0] // 2
        starts = [row_of(column[6][spot]) for spot in spots]
        table_w = jnp.concatenate(
            [
                window_rows(wy, starts[q], kind * wide, (kind + 1) * wide)
                for q in range(2)
                for kind in range(2)
            ],
            axis=0,
        ).astype(jnp.bfloat16)[:, :deep]
        mixed = jnp.dot(
            table_w,
            jnp.concatenate([high, high, rest], axis=0),
            preferred_element_type=jnp.float32,
        )
        fronts = []
        for kind in range(2):
            pieces = []
            for i in range(WIN):
                where = slice(i * lanes_all, (i + 1) * lanes_all)
                pieces.append(
                    jnp.where(
                        low_w,
                        mixed[kind * WIN : (kind + 1) * WIN, where],
                        mixed[(2 + kind) * WIN : (3 + kind) * WIN, where],
                    )
                )
            fronts.append(jnp.concatenate(pieces, axis=0))
        starts = [row_of(column[7][spot] + column[1][spot] - column[4][spot]) for spot in spots]
        table_w = jnp.concatenate(
            [
                window_rows(wx, starts[q], q * (wx.shape[0] // 2), (q + 1) * (wx.shape[0] // 2))
                for q in range(2)
            ],
            axis=0,
        )
        values = lax.dot_general(
            jnp.concatenate(fronts, axis=1),
            table_w,
            (((1,), (1,)), ((), ())),
            precision=PRECISE,
            preferred_element_type=jnp.float32,
        )
        line = lax.broadcasted_iota(jnp.int32, values.shape, 0)
        lane = lax.broadcasted_iota(jnp.int32, values.shape, 1)
        low_v = lane < WIN
        values = values * jnp.where(
            low_v, alive[spots[0]].astype(jnp.float32), alive[spots[1]].astype(jnp.float32)
        )
        weight = values * values
        places = (line // WIN, line % WIN, lane % WIN)
        long = corr_ref.shape[1]
        place_row = lax.broadcasted_iota(jnp.int32, (2 * WIN, long), 0)
        place_lane = lax.broadcasted_iota(jnp.int32, (2 * WIN, long), 1)
        spread_row = lax.broadcasted_iota(jnp.int32, (WIN * WIN, long), 0)
        spread_lane = lax.broadcasted_iota(jnp.int32, (WIN * WIN, long), 1)
        for q, spot in enumerate(spots):
            mask = low_v if q == 0 else jnp.logical_not(low_v)
            mine = jnp.where(mask, weight, 0.0)
            energy = jnp.sum(mine, keepdims=True) / total_cells
            shifts = [
                (
                    jnp.sum(mine * where.astype(jnp.float32), keepdims=True) / total_cells
                    + energy * column[5 + axis][spot].astype(jnp.float32)
                )
                / (energy + EPSILON)
                for axis, where in enumerate(places)
            ]
            pick = (place_row == place_lane % WIN + q * WIN).astype(jnp.float32)
            spread = jnp.dot(
                values, pick, precision=PRECISE, preferred_element_type=jnp.float32
            )
            line_out = jnp.sum(
                jnp.where(spread_lane // WIN == spread_row, spread, 0.0), axis=0, keepdims=True
            )
            slot_row = lax.broadcasted_iota(jnp.int32, corr_ref.shape, 0)
            corr_all = jnp.where(slot_row == slots[spot], line_out, corr_all)

            spot_row = lax.broadcasted_iota(jnp.int32, shift_ref.shape, 0)
            spot_lane = lax.broadcasted_iota(jnp.int32, shift_ref.shape, 1)
            for axis in range(3):
                shift_all = jnp.where(
                    (spot_row == axis) & (spot_lane == slots[spot]), shifts[axis], shift_all
                )

            view = lax.broadcasted_iota(jnp.int32, part.shape, 0)
            entry = lax.broadcasted_iota(jnp.int32, part.shape, 1)
            center_z = (own.astype(jnp.float32) * edge + 0.5 * edge) / float(edge * slab_count)
            center_x = (column[1][spot].astype(jnp.float32) + 0.5 * edge) / (2.0 * edge)

            def center(index, center_z=center_z, center_x=center_x):
                return jnp.where(
                    index == 0,
                    center_z,
                    jnp.where(index == 1, 0.5, jnp.where(index == 2, center_x, 1.0)),
                )

            hit_a = (view == column[0][spot]).astype(jnp.float32)
            hit_b = (view == column[2][spot]).astype(jnp.float32)
            block, spot_in = entry // 8, entry % 8
            normal = (hit_a + hit_b) * center(block) * center(spot_in)
            shift = jnp.where(block == 4, shifts[0], jnp.where(block == 5, shifts[1], shifts[2]))
            rhs = (hit_a - hit_b) * center(spot_in) * shift
            sums_all = sums_all + jnp.where(
                block < 4, normal, jnp.where(block < 7, rhs, 0.0)
            ) * (energy / float(cap * slab_count))

    part[...] = sums_all
    corr_ref[...] = corr_all
    shift_ref[...] = shift_all

    def part_copy(peer, source):
        return pltpu.make_async_remote_copy(
            src_ref=part,
            dst_ref=parts.at[source],
            send_sem=sum_send.at[peer],
            recv_sem=sum_recv.at[source],
            device_id={"slab": peer},
            device_id_type=pl.DeviceIdType.MESH,
        )

    def send_part(step, _):
        part_copy(lax.rem(own + step, slab_count), own).start()
        return 0

    lax.fori_loop(1, slab_count, send_part, 0)
    parts[own] = part[...]
    for side in range(2):
        on(side, lambda side=side: list_copy(side).wait_send())
    for item in items:
        on(item[0], lambda item=item: block_copy(*item).wait_send())

    def wait_part(step, _):
        peer = lax.rem(own + step, slab_count)
        part_copy(peer, own).wait_send()
        part_copy(peer, peer).wait_recv()
        return 0

    lax.fori_loop(1, slab_count, wait_part, 0)
    sums_ref[...] = lax.fori_loop(
        1, slab_count, lambda index, total: total + parts[index], parts[0]
    )


def fused(volumes, pair_fields, pair_counts, slab_count):
    views, edge = volumes.shape[0], volumes.shape[1]
    cap = pair_fields.shape[0]
    lanes = 2 * edge
    half = edge // 2
    kept = padded(edge)
    tables = static_tables(edge)
    vmem = pl.BlockSpec(memory_space=pltpu.VMEM)
    hbm = pl.BlockSpec(memory_space=pltpu.HBM)
    f32, bf16 = jnp.float32, jnp.bfloat16
    spectrum = (half + 1, edge, lanes)
    return pl.pallas_call(
        functools.partial(fused_kernel, slab_count),
        out_shape=(
            jax.ShapeDtypeStruct((cap, WIN**3), f32),
            jax.ShapeDtypeStruct((8, lanes), f32),
            jax.ShapeDtypeStruct((views, lanes), f32),
        ),
        in_specs=[hbm] * (3 + len(tables)),
        out_specs=(vmem, vmem, vmem),
        scratch_shapes=[
            pltpu.SMEM(pair_fields.shape, jnp.int32),
            pltpu.SMEM(pair_counts.shape, jnp.int32),
            pltpu.VMEM(volumes.shape, bf16),
        ]
        + [pltpu.VMEM(table.shape, table.dtype) for table in tables]
        + [
            pltpu.VMEM((2, 1, lanes), jnp.int32),
            pltpu.SMEM((2, 1, lanes), jnp.int32),
            pltpu.VMEM((2, half, edge, lanes), bf16),
            pltpu.VMEM((2, half, edge, lanes), bf16),
            pltpu.VMEM((cap // 2, 4 * lanes, 2 * lanes), bf16),
            pltpu.VMEM((cap // 2, 2, 4 * lanes, 2 * lanes), bf16),
            pltpu.VMEM((2, edge * edge, lanes), bf16),
            pltpu.VMEM((2, edge * edge, lanes), bf16),
            pltpu.VMEM((kept * (edge + GAP), lanes), f32),
            pltpu.VMEM((kept * (edge + GAP), lanes), f32),
            pltpu.VMEM((cap // 2,) + spectrum, f32),
            pltpu.VMEM((cap // 2,) + spectrum, f32),
            pltpu.VMEM(spectrum, f32),
            pltpu.VMEM(spectrum, f32),
            pltpu.VMEM(spectrum, f32),
            pltpu.VMEM((kept * WIN, lanes), f32),
            pltpu.VMEM((kept * WIN, lanes), f32),
            pltpu.VMEM((views, lanes), f32),
            pltpu.VMEM((slab_count, views, lanes), f32),
            pltpu.SemaphoreType.DMA((2 + len(tables),)),
            pltpu.SemaphoreType.DMA((PIECES,)),
            pltpu.SemaphoreType.DMA((2,)),
            pltpu.SemaphoreType.DMA((2,)),
            pltpu.SemaphoreType.DMA((2, NBR, PIECES)),
            pltpu.SemaphoreType.DMA((2, NBR, PIECES)),
            pltpu.SemaphoreType.DMA((slab_count,)),
            pltpu.SemaphoreType.DMA((slab_count,)),
        ]
        + [pltpu.VMEM((2, half // PIECES, edge, lanes), bf16)] * (NBR * PIECES),
        compiler_params=pltpu.CompilerParams(
            collective_id=1, has_side_effects=True, vmem_limit_bytes=60 * 2**20
        ),
        name="fused",
    )(pair_fields, pair_counts, volumes, *[jnp.asarray(table) for table in tables])


def finish_kernel(corr_in, shift_in, sums_in, corr_ref, shift_ref, normal_ref, rhs_ref):
    views, lanes = sums_in.shape
    corr_ref[...] = corr_in[...]
    shift_ref[...] = shift_in[: shift_ref.shape[0], : shift_ref.shape[1]]
    turned = jnp.concatenate(
        [sums_in[...], jnp.zeros((lanes - views, lanes), jnp.float32)], axis=0
    ).T
    for index in range(4):
        normal_ref[index] = turned[8 * index : 8 * index + 4, :views]
    for index in range(3):
        rhs_ref[index] = turned[32 + 8 * index : 36 + 8 * index, :views]


def finished(corr, shifts, sums):
    cap, views = corr.shape[0], sums.shape[0]
    vmem = pl.BlockSpec(memory_space=pltpu.VMEM)
    f32 = jnp.float32
    return pl.pallas_call(
        finish_kernel,
        out_shape=(
            jax.ShapeDtypeStruct(corr.shape, f32),
            jax.ShapeDtypeStruct((3, cap), f32),
            jax.ShapeDtypeStruct((4, 4, views), f32),
            jax.ShapeDtypeStruct((3, 4, views), f32),
        ),
        in_specs=[vmem] * 3,
        out_specs=(vmem,) * 4,
        name="finish",
    )(corr, shifts, sums)


def on_device(volumes, pair_fields, pair_counts):
    slab_count = lax.axis_size("slab")
    corr, shifts, sums = fused(volumes, pair_fields.T, pair_counts, slab_count)
    corr, shifts, normal, rhs = finished(corr, shifts, sums)
    return corr, shifts, normal.transpose(2, 0, 1), rhs.transpose(2, 1, 0)


def solution(mesh):
    in_specs = (P("tm", "slab", None, None), P(None, ("tm", "slab")), P(("tm", "slab")))
    out_specs = (
        P(("tm", "slab"), None),
        P(None, ("tm", "slab")),
        P("tm", None, None),
        P("tm", None, None),
    )
    return jax.shard_map(
        on_device, mesh=mesh, in_specs=in_specs, out_specs=out_specs, check_vma=False
    )
```

```python
import functools

import jax
import jax.numpy as jnp
import numpy as np
from jax import lax
from jax.experimental import pallas as pl
from jax.experimental.pallas import tpu as pltpu
from jax.sharding import PartitionSpec as P

WIN = 8
NBR = 2
EPSILON = 1e-06
SMALL = 1e-37
GAP = 4
PIECES = 5
LOADS = 4
PRECISE = lax.Precision.HIGHEST


def halves(table):
    table = table.astype(np.float32)
    high = table.astype(jnp.bfloat16)
    low = (table - high.astype(np.float32)).astype(jnp.bfloat16)
    return high, low


def three(table):
    high, low = halves(table)
    return np.concatenate([high, low, high], axis=1)


def cuts(half):
    return (0, half // 16, 3 * half // 8, 3 * half // 4, 15 * half // 16, half)


def padded(edge):
    return (edge // 2 + 1 + 7) // 8 * 8


def tiled(table):
    return np.ascontiguousarray(table.reshape(table.shape[0], -1, 128).transpose(1, 0, 2))


def static_tables(edge):
    half = edge // 2
    kept = padded(edge)
    ids = np.arange(edge)
    cells = np.arange(2 * edge) % edge
    angles = 2 * np.pi * (np.outer(cells, ids) % edge) / edge
    cos, sin, none = np.cos(angles), np.sin(angles), np.zeros((2 * edge, edge))
    table_x = np.concatenate(
        [
            np.concatenate([cos, none, -sin, none], axis=1),
            np.concatenate([none, cos, none, -sin], axis=1),
        ],
        axis=0,
    )
    table_x = np.concatenate(halves(table_x), axis=0).astype(np.float32)

    angles = 2 * np.pi * (np.outer(ids, ids) % edge) / edge
    cos, sin = np.cos(angles), np.sin(angles)
    table_z = three(np.block([[cos, sin], [-sin, cos]]))
    table_y = np.zeros((2 * kept, 2 * edge))
    table_y[: half + 1] = np.concatenate([cos, sin], axis=1)[: half + 1]
    table_y[kept : kept + half + 1] = np.concatenate([-sin, cos], axis=1)[: half + 1]
    table_y = three(table_y)

    steps = np.arange(edge + WIN) % edge
    angles = 2 * np.pi * (np.outer(steps, ids) % edge) / edge
    cos, sin = np.cos(angles), np.sin(angles)
    win_z = np.concatenate(
        [three(np.concatenate([cos, -sin], axis=1)), three(np.concatenate([sin, cos], axis=1))],
        axis=1,
    ).astype(np.float32)
    times = np.zeros((kept,))
    times[: half + 1] = 2.0
    times[0] = times[half] = 1.0
    cos_y = np.zeros((edge + WIN, kept))
    sin_y = np.zeros((edge + WIN, kept))
    cos_y[:, : half + 1] = cos[:, : half + 1]
    sin_y[:, : half + 1] = sin[:, : half + 1]
    cos_y, sin_y = cos_y * times, sin_y * times
    parts = []
    for part in ([cos_y, -sin_y], [sin_y, cos_y]):
        part = three(np.concatenate(part, axis=1)).astype(np.float32)
        extra = -part.shape[1] % 128
        parts.append(np.pad(part, ((0, 0), (0, extra))))
    win_y = np.concatenate(parts, axis=1)
    scale = edge**-1.5
    none = np.zeros_like(cos)
    win_x = np.concatenate(
        [cos * scale, none, -sin * scale, none, none, cos * scale, none, -sin * scale], axis=1
    ).astype(np.float32)
    return table_x, table_y, table_z, tiled(win_z), tiled(win_y), tiled(win_x)


def split(values):
    high = values.astype(jnp.bfloat16)
    return high, (values - high.astype(jnp.float32)).astype(jnp.bfloat16)


def fused_kernel(
    slab_count,
    fields_hbm,
    counts_hbm,
    volumes_hbm,
    tx_hbm,
    ty_hbm,
    tz_hbm,
    wz_hbm,
    wy_hbm,
    wx_hbm,
    corr_ref,
    shift_ref,
    sums_ref,
    fields_ref,
    counts_ref,
    held,
    tx,
    ty,
    tz,
    wz,
    wy,
    wx,
    request,
    asked,
    packed_first,
    packed_second,
    table_a,
    table_b,
    x_high,
    x_rest,
    y_re,
    y_im,
    a_re,
    a_im,
    c_re,
    c_im,
    c_abs,
    g_re,
    g_im,
    part,
    parts,
    local_sems,
    load_sems,
    list_send,
    list_recv,
    send_sems,
    recv_sems,
    sum_send,
    sum_recv,
    *landed,
):
    edge = held.shape[1]
    lanes_all = 2 * edge
    half = edge // 2
    kept = padded(edge)
    pitch = edge + GAP
    cap = fields_ref.shape[0]
    views = held.shape[0]
    batches = cap // 2
    bounds = cuts(half)
    cells = [last - first for first, last in zip(bounds, bounds[1:])]
    own = lax.axis_index("slab")
    packed = (packed_first, packed_second)
    got = (landed[:PIECES], landed[PIECES:])

    small = [
        pltpu.make_async_copy(src, dst, local_sems.at[index])
        for index, (src, dst) in enumerate(
            (
                (fields_hbm, fields_ref),
                (counts_hbm, counts_ref),
                (tx_hbm, tx),
                (ty_hbm, ty),
                (tz_hbm, tz),
                (wz_hbm, wz),
                (wy_hbm, wy),
                (wx_hbm, wx),
            )
        )
    ]
    for copy in small:
        copy.start()
    step_z = edge // LOADS
    loads = [
        pltpu.make_async_copy(
            volumes_hbm.at[:, pl.ds(piece * step_z, step_z)],
            held.at[:, pl.ds(piece * step_z, step_z)],
            load_sems.at[piece],
        )
        for piece in range(LOADS)
    ]
    for copy in loads:
        copy.start()

    for side in range(2):
        for index in range(2 * NBR):
            asked[side, 0, index] = 0
    present = (own > 0, own < slab_count - 1)
    peers = (lax.rem(own + slab_count - 1, slab_count), lax.rem(own + 1, slab_count))

    def on(side, action):
        pl.when(present[side])(action)

    barrier = pltpu.get_barrier_semaphore()

    def greet(step, _):
        pl.semaphore_signal(
            barrier,
            inc=1,
            device_id={"slab": lax.rem(own + step, slab_count)},
            device_id_type=pl.DeviceIdType.MESH,
        )
        return 0

    lax.fori_loop(1, slab_count, greet, 0)

    small[0].wait()
    small[1].wait()
    count = counts_ref[0, 0]
    live = [count > slot for slot in range(cap)]
    direction = [jnp.where(live[slot], fields_ref[slot, 3], 0) for slot in range(cap)]
    rank = []
    for slot in range(cap):
        seen = jnp.int32(0)
        for other in range(slot):
            seen = seen + (direction[other] == direction[slot]).astype(jnp.int32)
        rank.append(jnp.where(direction[slot] == 0, 0, seen))
    late = [(rank[slot] > 0).astype(jnp.int32) for slot in range(cap)]
    early_total = cap - sum(late)
    place = []
    early_seen, late_seen = jnp.int32(0), jnp.int32(0)
    for slot in range(cap):
        place.append(jnp.where(late[slot] > 0, early_total + late_seen, early_seen))
        early_seen = early_seen + 1 - late[slot]
        late_seen = late_seen + late[slot]

    def ordered(values):
        result = []
        for spot in range(cap):
            value = jnp.int32(0)
            for slot in range(cap):
                value = jnp.where(place[slot] == spot, values[slot], value)
            result.append(value)
        return result

    column = [
        ordered([jnp.where(live[slot], fields_ref[slot, row], 0) for slot in range(cap)])
        for row in range(8)
    ]
    slots = ordered([jnp.int32(slot) for slot in range(cap)])
    alive = ordered([live[slot].astype(jnp.int32) for slot in range(cap)])
    ranks = ordered(rank)

    lane8 = lax.broadcasted_iota(jnp.int32, request.shape[1:], 1)
    for side, wanted in enumerate((-1, 1)):
        values = jnp.zeros(request.shape[1:], jnp.int32)
        for level in range(NBR):
            view, anchor = jnp.int32(0), jnp.int32(0)
            for slot in range(cap):
                take = (direction[slot] == wanted) & (rank[slot] == level)
                view = jnp.where(take, fields_ref[slot, 2], view)
                anchor = jnp.where(take, fields_ref[slot, 4], anchor)
            values = jnp.where(lane8 == 2 * level, view, values)
            values = jnp.where(lane8 == 2 * level + 1, anchor, values)
        request[side] = values

    pl.semaphore_wait(barrier, slab_count - 1)

    def list_copy(side):
        return pltpu.make_async_remote_copy(
            src_ref=request.at[side],
            dst_ref=asked.at[1 - side],
            send_sem=list_send.at[side],
            recv_sem=list_recv.at[1 - side],
            device_id={"slab": peers[side]},
            device_id_type=pl.DeviceIdType.MESH,
        )

    def list_arrival(side):
        return pltpu.make_async_remote_copy(
            src_ref=request.at[side],
            dst_ref=asked.at[side],
            send_sem=list_send.at[side],
            recv_sem=list_recv.at[side],
            device_id={"slab": peers[side]},
            device_id_type=pl.DeviceIdType.MESH,
        )

    for side in range(2):
        on(side, lambda side=side: list_copy(side).start())

    for copy in small[2:]:
        copy.wait()
    rows = lax.broadcasted_iota(jnp.int32, (lanes_all, lanes_all), 0)

    def fill(table, starts):
        for piece in range(4):
            where = pl.ds(piece * lanes_all, lanes_all)
            start = starts[piece % 2]
            inside = (rows >= start) & (rows < start + edge)
            for side in range(2):
                cols = pl.ds(side * lanes_all, lanes_all)
                table[where, cols] = jnp.where(inside, tx[where, cols], 0.0).astype(jnp.bfloat16)

    for batch in range(batches):
        fill(table_a.at[batch], column[1][2 * batch : 2 * batch + 2])
        for part_z in range(2):
            fill(
                table_b.at[batch, part_z],
                [
                    jnp.where(column[3][spot] == 0, column[4][spot], part_z * edge)
                    for spot in range(2 * batch, 2 * batch + 2)
                ],
            )

    for side in range(2):
        on(side, lambda side=side: list_arrival(side).wait_recv())
    for copy in loads:
        copy.wait()

    def pack_piece(side, level, piece):
        view = asked[side, 0, 2 * level]
        anchor = asked[side, 0, 2 * level + 1]

        def step(index, _):
            z = bounds[piece] + index
            lanes = lax.broadcasted_iota(jnp.int32, (edge, lanes_all), 1)
            low = lanes < edge
            first = held[view, z].astype(jnp.float32)
            second = held[view, half + z].astype(jnp.float32)
            straight = jnp.where(low, first, second)
            turned = pltpu.roll(jnp.where(low, second, first), edge, 1)
            keep = (low & (lanes >= anchor)) | ((lanes >= edge) & (lanes < edge + anchor))
            packed[level][side, z] = jnp.where(keep, straight, turned).astype(jnp.bfloat16)
            return 0

        lax.fori_loop(0, cells[piece], step, 0, unroll=True)

    def block_copy(side, level, piece):
        where = pl.ds(bounds[piece], cells[piece])
        peer = lax.rem(own + slab_count + 2 * side - 1, slab_count)
        return pltpu.make_async_remote_copy(
            src_ref=packed[level].at[side, where],
            dst_ref=got[level][piece].at[side],
            send_sem=send_sems.at[side, level, piece],
            recv_sem=recv_sems.at[side, level, piece],
            device_id={"slab": peer},
            device_id_type=pl.DeviceIdType.MESH,
        )

    def block_arrival(side, level, piece):
        where = pl.ds(bounds[piece], cells[piece])
        return pltpu.make_async_remote_copy(
            src_ref=packed[level].at[side, where],
            dst_ref=got[level][piece].at[1 - side],
            send_sem=send_sems.at[side, level, piece],
            recv_sem=recv_sems.at[1 - side, level, piece],
            device_id={"slab": peers[side]},
            device_id_type=pl.DeviceIdType.MESH,
        )

    items = [
        (side, level, piece)
        for level in range(NBR)
        for piece in range(PIECES)
        for side in range(2)
    ]
    away = lax.rem(own, 2)
    odd = lax.rem(own, 4) * (3 - lax.rem(own, 4)) == 0
    there = (
        jnp.where(away == 0, present[0], present[1]),
        jnp.where(away == 0, present[1], present[0]),
    )

    def send(turn, level, piece):
        side = away if turn == 0 else 1 - away
        pl.when(there[turn])(lambda: block_copy(side, level, piece).start())

    def send_later(moment):
        for turn in range(2):
            late_here = odd & (turn == 0)

            @pl.when(there[turn] & (late_here if moment else jnp.logical_not(late_here)))
            def _(turn=turn):
                side = away if turn == 0 else 1 - away
                for level in range(1, NBR):
                    for piece in range(PIECES):
                        block_copy(side, level, piece).start()

    def pack_level(level, start):
        mine = [(turn, level, piece) for turn in range(2) for piece in range(PIECES)]
        for number, (turn, _, piece) in enumerate(mine):
            pack_piece(away if turn == 0 else 1 - away, level, piece)
            if number and start:
                send(*mine[number - 1])
        if start:
            send(*mine[-1])

    pack_level(0, True)

    lanes = lax.broadcasted_iota(jnp.int32, (edge, lanes_all), 1)
    low = lanes < edge

    def x_planes(left, right, table, z, planes):
        sides = jnp.concatenate(
            [
                left.reshape(planes * edge, lanes_all),
                right.reshape(planes * edge, lanes_all),
            ],
            axis=1,
        )
        mixed = jnp.dot(
            jnp.concatenate([sides, sides], axis=1), table, preferred_element_type=jnp.float32
        )
        high, rest = split(mixed)
        where = pl.ds(z * edge, planes * edge)
        for side in range(2):
            cols = slice(side * lanes_all, (side + 1) * lanes_all)
            x_high[side, where, :] = high[:, cols]
            x_rest[side, where, :] = rest[:, cols]

    def y_planes(z, planes):
        def planar(ref, side):
            return jnp.concatenate(
                [ref[side, pl.ds((z + k) * edge, edge), :] for k in range(planes)], axis=1
            )

        highs = [planar(x_high, 0), planar(x_high, 1)]
        rests = [planar(x_rest, 0), planar(x_rest, 1)]
        mixed = jnp.dot(
            ty[...],
            jnp.concatenate(highs + highs + rests, axis=0),
            preferred_element_type=jnp.float32,
        )
        for index in range(planes):
            where = slice(index * lanes_all, (index + 1) * lanes_all)
            spots = pl.ds(z + index, half + 1, stride=pitch)
            y_re[spots, :] = mixed[: half + 1, where]
            y_im[spots, :] = mixed[kept : kept + half + 1, where]

    def z_plane(ky):
        where = pl.ds(ky * pitch, edge)
        real = split(y_re[where, :])
        imag = split(y_im[where, :])
        return [real[0], imag[0], real[0], imag[0], real[1], imag[1]]

    def z_planes(kys):
        stacks = [z_plane(ky) for ky in kys]
        mixed = jnp.dot(
            tz[...],
            jnp.concatenate(
                [jnp.concatenate([s[k] for s in stacks], axis=1) for k in range(6)], axis=0
            ),
            preferred_element_type=jnp.float32,
        )
        return [
            (
                mixed[:edge, k * lanes_all : (k + 1) * lanes_all],
                mixed[edge:, k * lanes_all : (k + 1) * lanes_all],
            )
            for k in range(len(kys))
        ]

    chunk = edge // 4
    for batch in range(batches):
        views_a = column[0][2 * batch : 2 * batch + 2]

        def first_x(step, batch=batch, views_a=views_a):
            z = chunk * step
            x_planes(
                held[views_a[0], pl.ds(z, chunk)],
                held[views_a[1], pl.ds(z, chunk)],
                table_a[batch],
                z,
                chunk,
            )

        def first_step(step, _, first_x=first_x):
            y_planes(chunk * step, chunk)
            first_x(step + 1)
            return 0

        first_x(0)
        lax.fori_loop(0, edge // chunk - 1, first_step, 0)
        y_planes(edge - chunk, chunk)

        def first_z(step, _, batch=batch):
            for ky, (real, imag) in zip(
                (2 * step, 2 * step + 1), z_planes((2 * step, 2 * step + 1))
            ):
                a_re[batch, ky] = real
                a_im[batch, ky] = imag
            return 0

        lax.fori_loop(0, half // 2, first_z, 0, unroll=4)
        ((real, imag),) = z_planes((half,))
        a_re[batch, half] = real
        a_im[batch, half] = imag
        if batch == 0:
            for level in range(1, NBR):
                pack_level(level, False)

    send_later(0)

    g_re[pl.ds((half + 1) * WIN, (kept - half - 1) * WIN), :] = jnp.zeros(
        ((kept - half - 1) * WIN, lanes_all), jnp.float32
    )
    g_im[pl.ds((half + 1) * WIN, (kept - half - 1) * WIN), :] = jnp.zeros(
        ((kept - half - 1) * WIN, lanes_all), jnp.float32
    )

    total_cells = float(WIN**3)
    found = []
    shift_all = jnp.zeros(shift_ref.shape, jnp.float32)
    sums_all = jnp.zeros(part.shape, jnp.float32)

    for batch in range(batches):
        spots = (2 * batch, 2 * batch + 1)
        local = [column[3][spot] == 0 for spot in spots]
        which = [jnp.where(column[3][spot] < 0, 1, 0) for spot in spots]

        def second(q, piece, part_z, spots=spots, local=local, which=which, batch=batch):
            start = part_z * half + bounds[piece]
            inner = held[column[2][spots[q]], pl.ds(start, cells[piece])]
            outer = got[0][piece][which[q]]
            if batch:
                outer = jnp.where(ranks[spots[q]] > 0, got[1][piece][which[q]], outer)
            return jnp.where(local[q], inner, outer)

        for piece in range(PIECES):
            for side in range(2):
                on(
                    side,
                    lambda side=side, piece=piece: block_arrival(side, batch, piece).wait_recv(),
                )
            for part_z in range(2):
                x_planes(
                    second(0, piece, part_z),
                    second(1, piece, part_z),
                    table_b[batch, part_z],
                    part_z * half + bounds[piece],
                    cells[piece],
                )
            for part_z in range(2):
                if piece:
                    y_planes(part_z * half + bounds[piece - 1], cells[piece - 1])
            if batch == 0 and piece == PIECES - 3:
                send_later(1)
        for part_z in range(2):
            y_planes(part_z * half + bounds[PIECES - 1], cells[PIECES - 1])

        def cross_plane(ky, real, imag, total, batch=batch):
            front_re, front_im = a_re[batch, ky], a_im[batch, ky]
            cross_re = front_re * real + front_im * imag
            cross_im = front_im * real - front_re * imag
            square = cross_re * cross_re + cross_im * cross_im
            size = square * lax.rsqrt(jnp.maximum(square, SMALL))
            c_re[ky] = cross_re
            c_im[ky] = cross_im
            c_abs[ky] = size
            return total + size

        def second_z(step, total, batch=batch):
            kys = (2 * step, 2 * step + 1)
            for ky, (real, imag) in zip(kys, z_planes(kys)):
                total = cross_plane(ky, real, imag, total)
            return total

        total = lax.fori_loop(
            0, half // 2, second_z, jnp.zeros((edge, lanes_all), jnp.float32), unroll=4
        )
        ((real, imag),) = z_planes((half,))
        total = 2.0 * cross_plane(half, real, imag, total) - c_abs[0] - c_abs[half]
        floors = [
            jnp.sum(jnp.where(mask, total, 0.0)) / float(edge**3) + EPSILON
            for mask in (low, jnp.logical_not(low))
        ]
        floor = jnp.where(low, floors[0], floors[1])

        def row_of(value):
            return lax.rem(value + 4 * edge, edge)

        def window_rows(ref, start, first, last):
            return jnp.concatenate(
                [ref[k, pl.ds(start, WIN), :] for k in range(first, last)], axis=1
            )

        wide = wz.shape[0] // 2
        starts = [row_of(column[5][spot]) for spot in spots]
        table_w = jnp.concatenate(
            [
                window_rows(wz, starts[q], kind * wide, (kind + 1) * wide)
                for q in range(2)
                for kind in range(2)
            ],
            axis=0,
        ).astype(jnp.bfloat16)
        low_w = low[:WIN]

        def window_planes(kys, floor=floor, table_w=table_w):
            stacks = []
            for ky in kys:
                size = c_abs[ky] + floor
                inverse = pl.reciprocal(size, approx=True)
                inverse = inverse * (2.0 - size * inverse)
                real = split(c_re[ky] * inverse)
                imag = split(c_im[ky] * inverse)
                stacks.append([real[0], imag[0], real[0], imag[0], real[1], imag[1]])
            mixed = jnp.dot(
                table_w,
                jnp.concatenate(
                    [jnp.concatenate([s[k] for s in stacks], axis=1) for k in range(6)], axis=0
                ),
                preferred_element_type=jnp.float32,
            )
            for k, ky in enumerate(kys):
                cut = mixed[:, k * lanes_all : (k + 1) * lanes_all]
                where = pl.ds(pl.multiple_of(ky * WIN, 8), WIN)
                g_re[where, :] = jnp.where(low_w, cut[:WIN], cut[2 * WIN : 3 * WIN])
                g_im[where, :] = jnp.where(low_w, cut[WIN : 2 * WIN], cut[3 * WIN :])

        def window_step(step, _):
            window_planes((2 * step, 2 * step + 1))
            return 0

        lax.fori_loop(0, half // 2, window_step, 0, unroll=4)
        window_planes((half,))

        stack = jnp.concatenate(
            [
                jnp.concatenate(
                    [ref[pl.ds(i, kept, stride=WIN), :] for i in range(WIN)], axis=1
                )
                for ref in (g_re, g_im)
            ],
            axis=0,
        )
        high, rest = split(stack)
        deep = 6 * kept
        wide = wy.shape[0] // 2
        starts = [row_of(column[6][spot]) for spot in spots]
        table_w = jnp.concatenate(
            [
                window_rows(wy, starts[q], kind * wide, (kind + 1) * wide)
                for q in range(2)
                for kind in range(2)
            ],
            axis=0,
        ).astype(jnp.bfloat16)[:, :deep]
        mixed = jnp.dot(
            table_w,
            jnp.concatenate([high, high, rest], axis=0),
            preferred_element_type=jnp.float32,
        )
        fronts = []
        for kind in range(2):
            pieces = []
            for i in range(WIN):
                where = slice(i * lanes_all, (i + 1) * lanes_all)
                pieces.append(
                    jnp.where(
                        low_w,
                        mixed[kind * WIN : (kind + 1) * WIN, where],
                        mixed[(2 + kind) * WIN : (3 + kind) * WIN, where],
                    )
                )
            fronts.append(jnp.concatenate(pieces, axis=0))
        starts = [row_of(column[7][spot] + column[1][spot] - column[4][spot]) for spot in spots]
        table_w = jnp.concatenate(
            [
                window_rows(wx, starts[q], q * (wx.shape[0] // 2), (q + 1) * (wx.shape[0] // 2))
                for q in range(2)
            ],
            axis=0,
        )
        values = lax.dot_general(
            jnp.concatenate(fronts, axis=1),
            table_w,
            (((1,), (1,)), ((), ())),
            precision=PRECISE,
            preferred_element_type=jnp.float32,
        )
        line = lax.broadcasted_iota(jnp.int32, values.shape, 0)
        lane = lax.broadcasted_iota(jnp.int32, values.shape, 1)
        low_v = lane < WIN
        values = values * jnp.where(
            low_v, alive[spots[0]].astype(jnp.float32), alive[spots[1]].astype(jnp.float32)
        )
        weight = values * values
        places = (line // WIN, line % WIN, lane % WIN)
        found.append(values)
        for q, spot in enumerate(spots):
            mask = low_v if q == 0 else jnp.logical_not(low_v)
            mine = jnp.where(mask, weight, 0.0)
            energy = jnp.sum(mine, keepdims=True) / total_cells
            shifts = [
                (
                    jnp.sum(mine * where.astype(jnp.float32), keepdims=True) / total_cells
                    + energy * column[5 + axis][spot].astype(jnp.float32)
                )
                / (energy + EPSILON)
                for axis, where in enumerate(places)
            ]
            spot_row = lax.broadcasted_iota(jnp.int32, shift_ref.shape, 0)
            spot_lane = lax.broadcasted_iota(jnp.int32, shift_ref.shape, 1)
            for axis in range(3):
                shift_all = jnp.where(
                    (spot_row == axis) & (spot_lane == slots[spot]), shifts[axis], shift_all
                )

            view = lax.broadcasted_iota(jnp.int32, part.shape, 0)
            entry = lax.broadcasted_iota(jnp.int32, part.shape, 1)
            center_z = (own.astype(jnp.float32) * edge + 0.5 * edge) / float(edge * slab_count)
            center_x = (column[1][spot].astype(jnp.float32) + 0.5 * edge) / (2.0 * edge)

            def center(index, center_z=center_z, center_x=center_x):
                return jnp.where(
                    index == 0,
                    center_z,
                    jnp.where(index == 1, 0.5, jnp.where(index == 2, center_x, 1.0)),
                )

            hit_a = (view == column[0][spot]).astype(jnp.float32)
            hit_b = (view == column[2][spot]).astype(jnp.float32)
            block, spot_in = entry // 8, entry % 8
            normal = (hit_a + hit_b) * center(block) * center(spot_in)
            shift = jnp.where(block == 4, shifts[0], jnp.where(block == 5, shifts[1], shifts[2]))
            rhs = (hit_a - hit_b) * center(spot_in) * shift
            sums_all = sums_all + jnp.where(
                block < 4, normal, jnp.where(block < 7, rhs, 0.0)
            ) * (energy / float(cap * slab_count))

    part[...] = sums_all
    shift_ref[...] = shift_all

    def part_copy(peer, source):
        return pltpu.make_async_remote_copy(
            src_ref=part,
            dst_ref=parts.at[source],
            send_sem=sum_send.at[peer],
            recv_sem=sum_recv.at[source],
            device_id={"slab": peer},
            device_id_type=pl.DeviceIdType.MESH,
        )

    def send_part(step, _):
        part_copy(lax.rem(own + step, slab_count), own).start()
        return 0

    lax.fori_loop(1, slab_count, send_part, 0)
    parts[own] = part[...]

    long = corr_ref.shape[1]
    place_row = lax.broadcasted_iota(jnp.int32, (2 * WIN, long), 0)
    place_lane = lax.broadcasted_iota(jnp.int32, (2 * WIN, long), 1)
    spread_row = lax.broadcasted_iota(jnp.int32, (WIN * WIN, long), 0)
    spread_lane = lax.broadcasted_iota(jnp.int32, (WIN * WIN, long), 1)
    slot_row = lax.broadcasted_iota(jnp.int32, corr_ref.shape, 0)
    corr_all = jnp.zeros(corr_ref.shape, jnp.float32)
    for spot in range(cap):
        pick = (place_row == place_lane % WIN + spot % 2 * WIN).astype(jnp.float32)
        spread = jnp.dot(
            found[spot // 2], pick, precision=PRECISE, preferred_element_type=jnp.float32
        )
        row = jnp.sum(
            jnp.where(spread_lane // WIN == spread_row, spread, 0.0), axis=0, keepdims=True
        )
        corr_all = jnp.where(slot_row == slots[spot], row, corr_all)
    corr_ref[...] = corr_all
    for side in range(2):
        on(side, lambda side=side: list_copy(side).wait_send())
    for item in items:
        on(item[0], lambda item=item: block_copy(*item).wait_send())

    def wait_part(step, _):
        peer = lax.rem(own + step, slab_count)
        part_copy(peer, own).wait_send()
        part_copy(peer, peer).wait_recv()
        return 0

    lax.fori_loop(1, slab_count, wait_part, 0)
    sums_ref[...] = lax.fori_loop(
        1, slab_count, lambda index, total: total + parts[index], parts[0]
    )


def fused(volumes, pair_fields, pair_counts, slab_count):
    views, edge = volumes.shape[0], volumes.shape[1]
    cap = pair_fields.shape[0]
    lanes = 2 * edge
    half = edge // 2
    kept = padded(edge)
    tables = static_tables(edge)
    vmem = pl.BlockSpec(memory_space=pltpu.VMEM)
    hbm = pl.BlockSpec(memory_space=pltpu.HBM)
    f32, bf16 = jnp.float32, jnp.bfloat16
    spectrum = (half + 1, edge, lanes)
    return pl.pallas_call(
        functools.partial(fused_kernel, slab_count),
        out_shape=(
            pltpu.VMEM((cap, WIN**3), f32),
            pltpu.VMEM((8, lanes), f32),
            pltpu.VMEM((views, lanes), f32),
        ),
        in_specs=[hbm] * (3 + len(tables)),
        out_specs=(vmem, vmem, vmem),
        scratch_shapes=[
            pltpu.SMEM(pair_fields.shape, jnp.int32),
            pltpu.SMEM(pair_counts.shape, jnp.int32),
            pltpu.VMEM(volumes.shape, bf16),
        ]
        + [pltpu.VMEM(table.shape, table.dtype) for table in tables]
        + [
            pltpu.VMEM((2, 1, lanes), jnp.int32),
            pltpu.SMEM((2, 1, lanes), jnp.int32),
            pltpu.VMEM((2, half, edge, lanes), bf16),
            pltpu.VMEM((2, half, edge, lanes), bf16),
            pltpu.VMEM((cap // 2, 4 * lanes, 2 * lanes), bf16),
            pltpu.VMEM((cap // 2, 2, 4 * lanes, 2 * lanes), bf16),
            pltpu.VMEM((2, edge * edge, lanes), bf16),
            pltpu.VMEM((2, edge * edge, lanes), bf16),
            pltpu.VMEM((kept * (edge + GAP), lanes), f32),
            pltpu.VMEM((kept * (edge + GAP), lanes), f32),
            pltpu.VMEM((cap // 2,) + spectrum, f32),
            pltpu.VMEM((cap // 2,) + spectrum, f32),
            pltpu.VMEM(spectrum, f32),
            pltpu.VMEM(spectrum, f32),
            pltpu.VMEM(spectrum, f32),
            pltpu.VMEM((kept * WIN, lanes), f32),
            pltpu.VMEM((kept * WIN, lanes), f32),
            pltpu.VMEM((views, lanes), f32),
            pltpu.VMEM((slab_count, views, lanes), f32),
            pltpu.SemaphoreType.DMA((2 + len(tables),)),
            pltpu.SemaphoreType.DMA((LOADS,)),
            pltpu.SemaphoreType.DMA((2,)),
            pltpu.SemaphoreType.DMA((2,)),
            pltpu.SemaphoreType.DMA((2, NBR, PIECES)),
            pltpu.SemaphoreType.DMA((2, NBR, PIECES)),
            pltpu.SemaphoreType.DMA((slab_count,)),
            pltpu.SemaphoreType.DMA((slab_count,)),
        ]
        + [
            pltpu.VMEM((2, last - first, edge, lanes), bf16)
            for first, last in zip(cuts(half), cuts(half)[1:])
        ]
        * NBR,
        compiler_params=pltpu.CompilerParams(
            collective_id=1, has_side_effects=True, vmem_limit_bytes=60 * 2**20
        ),
        name="fused",
    )(pair_fields, pair_counts, volumes, *[jnp.asarray(table) for table in tables])


def finish_kernel(corr_in, shift_in, sums_in, corr_ref, shift_ref, normal_ref, rhs_ref):
    views, lanes = sums_in.shape
    corr_ref[...] = corr_in[...]
    shift_ref[...] = shift_in[: shift_ref.shape[0], : shift_ref.shape[1]]
    turned = jnp.concatenate(
        [sums_in[...], jnp.zeros((lanes - views, lanes), jnp.float32)], axis=0
    ).T
    for index in range(4):
        normal_ref[index] = turned[8 * index : 8 * index + 4, :views]
    for index in range(3):
        rhs_ref[index] = turned[32 + 8 * index : 36 + 8 * index, :views]


def finished(corr, shifts, sums):
    cap, views = corr.shape[0], sums.shape[0]
    vmem = pl.BlockSpec(memory_space=pltpu.VMEM)
    f32 = jnp.float32
    return pl.pallas_call(
        finish_kernel,
        out_shape=(
            jax.ShapeDtypeStruct(corr.shape, f32),
            jax.ShapeDtypeStruct((3, cap), f32),
            jax.ShapeDtypeStruct((4, 4, views), f32),
            jax.ShapeDtypeStruct((3, 4, views), f32),
        ),
        in_specs=[vmem] * 3,
        out_specs=(vmem,) * 4,
        name="finish",
    )(*[pltpu.with_memory_space_constraint(x, pltpu.VMEM) for x in (corr, shifts, sums)])


def on_device(volumes, pair_fields, pair_counts):
    slab_count = lax.axis_size("slab")
    corr, shifts, sums = fused(
        volumes, pair_fields.T, pair_counts.reshape(1, 1), slab_count
    )
    corr, shifts, normal, rhs = finished(corr, shifts, sums)
    return corr, shifts, normal.transpose(2, 0, 1), rhs.transpose(2, 1, 0)


def solution(mesh):
    in_specs = (P("tm", "slab", None, None), P(None, ("tm", "slab")), P(("tm", "slab")))
    out_specs = (
        P(("tm", "slab"), None),
        P(None, ("tm", "slab")),
        P("tm", None, None),
        P("tm", None, None),
    )
    return jax.shard_map(
        on_device, mesh=mesh, in_specs=in_specs, out_specs=out_specs, check_vma=False
    )
```

```python
import functools

import jax
import jax.numpy as jnp
import numpy as np
from jax import lax
from jax.experimental import pallas as pl
from jax.experimental.pallas import tpu as pltpu
from jax.sharding import PartitionSpec as P

WIN = 8
NBR = 2
EPSILON = 1e-06
SMALL = 1e-37
GAP = 4
PIECES = 6
LOADS = 4
PRECISE = lax.Precision.HIGHEST


def halves(table):
    table = table.astype(np.float32)
    high = table.astype(jnp.bfloat16)
    low = (table - high.astype(np.float32)).astype(jnp.bfloat16)
    return high, low


def three(table):
    high, low = halves(table)
    return np.concatenate([high, low, high], axis=1)


def cuts(half):
    return tuple(part * half // 16 for part in (0, 1, 3, 7, 12, 15, 16))


def padded(edge):
    return (edge // 2 + 1 + 7) // 8 * 8


def tiled(table):
    return np.ascontiguousarray(table.reshape(table.shape[0], -1, 128).transpose(1, 0, 2))


def static_tables(edge):
    half = edge // 2
    kept = padded(edge)
    ids = np.arange(edge)
    cells = np.arange(2 * edge) % edge
    angles = 2 * np.pi * (np.outer(cells, ids) % edge) / edge
    cos, sin, none = np.cos(angles), np.sin(angles), np.zeros((2 * edge, edge))
    table_x = np.concatenate(
        [
            np.concatenate([cos, none, -sin, none], axis=1),
            np.concatenate([none, cos, none, -sin], axis=1),
        ],
        axis=0,
    )
    table_x = np.concatenate(halves(table_x), axis=0).astype(np.float32)

    angles = 2 * np.pi * (np.outer(ids, ids) % edge) / edge
    cos, sin = np.cos(angles), np.sin(angles)
    table_z = three(np.block([[cos, sin], [-sin, cos]]))
    table_y = np.zeros((2 * kept, 2 * edge))
    table_y[: half + 1] = np.concatenate([cos, sin], axis=1)[: half + 1]
    table_y[kept : kept + half + 1] = np.concatenate([-sin, cos], axis=1)[: half + 1]
    table_y = three(table_y)

    steps = np.arange(edge + WIN) % edge
    angles = 2 * np.pi * (np.outer(steps, ids) % edge) / edge
    cos, sin = np.cos(angles), np.sin(angles)
    win_z = np.concatenate(
        [three(np.concatenate([cos, -sin], axis=1)), three(np.concatenate([sin, cos], axis=1))],
        axis=1,
    ).astype(np.float32)
    times = np.zeros((kept,))
    times[: half + 1] = 2.0
    times[0] = times[half] = 1.0
    cos_y = np.zeros((edge + WIN, kept))
    sin_y = np.zeros((edge + WIN, kept))
    cos_y[:, : half + 1] = cos[:, : half + 1]
    sin_y[:, : half + 1] = sin[:, : half + 1]
    cos_y, sin_y = cos_y * times, sin_y * times
    parts = []
    for part in ([cos_y, -sin_y], [sin_y, cos_y]):
        part = three(np.concatenate(part, axis=1)).astype(np.float32)
        extra = -part.shape[1] % 128
        parts.append(np.pad(part, ((0, 0), (0, extra))))
    win_y = np.concatenate(parts, axis=1)
    scale = edge**-1.5
    none = np.zeros_like(cos)
    win_x = np.concatenate(
        [cos * scale, none, -sin * scale, none, none, cos * scale, none, -sin * scale], axis=1
    ).astype(np.float32)
    return table_x, table_y, table_z, tiled(win_z), tiled(win_y), tiled(win_x)


def split(values):
    high = values.astype(jnp.bfloat16)
    return high, (values - high.astype(jnp.float32)).astype(jnp.bfloat16)


def fused_kernel(
    slab_count,
    fields_hbm,
    counts_hbm,
    volumes_hbm,
    tx_hbm,
    ty_hbm,
    tz_hbm,
    wz_hbm,
    wy_hbm,
    wx_hbm,
    corr_ref,
    shift_ref,
    sums_ref,
    fields_ref,
    counts_ref,
    held,
    tx,
    ty,
    tz,
    wz,
    wy,
    wx,
    request,
    asked,
    packed_first,
    packed_second,
    table_a,
    table_b,
    x_high,
    x_rest,
    y_re,
    y_im,
    a_re,
    a_im,
    c_re,
    c_im,
    c_abs,
    g_re,
    g_im,
    part,
    parts,
    local_sems,
    load_sems,
    list_send,
    list_recv,
    send_sems,
    recv_sems,
    sum_send,
    sum_recv,
    *landed,
):
    edge = held.shape[1]
    lanes_all = 2 * edge
    half = edge // 2
    kept = padded(edge)
    pitch = edge + GAP
    cap = fields_ref.shape[0]
    views = held.shape[0]
    batches = cap // 2
    bounds = cuts(half)
    cells = [last - first for first, last in zip(bounds, bounds[1:])]
    own = lax.axis_index("slab")
    packed = (packed_first, packed_second)
    got = (landed[:PIECES], landed[PIECES:])

    for side in range(2):
        for index in range(2 * NBR):
            asked[side, 0, index] = 0

    barrier = pltpu.get_barrier_semaphore()

    def greet(step, _):
        pl.semaphore_signal(
            barrier,
            inc=1,
            device_id={"slab": lax.rem(own + step, slab_count)},
            device_id_type=pl.DeviceIdType.MESH,
        )
        return 0

    lax.fori_loop(1, slab_count, greet, 0)

    small = [
        pltpu.make_async_copy(src, dst, local_sems.at[index])
        for index, (src, dst) in enumerate(
            (
                (fields_hbm, fields_ref),
                (counts_hbm, counts_ref),
                (tx_hbm, tx),
                (ty_hbm, ty),
                (tz_hbm, tz),
                (wz_hbm, wz),
                (wy_hbm, wy),
                (wx_hbm, wx),
            )
        )
    ]
    for copy in small:
        copy.start()
    step_z = edge // LOADS
    loads = [
        pltpu.make_async_copy(
            volumes_hbm.at[:, pl.ds(piece * step_z, step_z)],
            held.at[:, pl.ds(piece * step_z, step_z)],
            load_sems.at[piece],
        )
        for piece in range(LOADS)
    ]
    for copy in loads:
        copy.start()

    present = (own > 0, own < slab_count - 1)
    peers = (lax.rem(own + slab_count - 1, slab_count), lax.rem(own + 1, slab_count))

    def on(side, action):
        pl.when(present[side])(action)

    small[0].wait()
    small[1].wait()
    count = counts_ref[0, 0]
    live = [count > slot for slot in range(cap)]
    direction = [jnp.where(live[slot], fields_ref[slot, 3], 0) for slot in range(cap)]
    rank = []
    for slot in range(cap):
        seen = jnp.int32(0)
        for other in range(slot):
            seen = seen + (direction[other] == direction[slot]).astype(jnp.int32)
        rank.append(jnp.where(direction[slot] == 0, 0, seen))
    late = [(rank[slot] > 0).astype(jnp.int32) for slot in range(cap)]
    early_total = cap - sum(late)
    place = []
    early_seen, late_seen = jnp.int32(0), jnp.int32(0)
    for slot in range(cap):
        place.append(jnp.where(late[slot] > 0, early_total + late_seen, early_seen))
        early_seen = early_seen + 1 - late[slot]
        late_seen = late_seen + late[slot]

    def ordered(values):
        result = []
        for spot in range(cap):
            value = jnp.int32(0)
            for slot in range(cap):
                value = jnp.where(place[slot] == spot, values[slot], value)
            result.append(value)
        return result

    column = [
        ordered([jnp.where(live[slot], fields_ref[slot, row], 0) for slot in range(cap)])
        for row in range(8)
    ]
    slots = ordered([jnp.int32(slot) for slot in range(cap)])
    alive = ordered([live[slot].astype(jnp.int32) for slot in range(cap)])
    ranks = ordered(rank)

    lane8 = lax.broadcasted_iota(jnp.int32, request.shape[1:], 1)
    for side, wanted in enumerate((-1, 1)):
        values = jnp.zeros(request.shape[1:], jnp.int32)
        for level in range(NBR):
            view, anchor = jnp.int32(0), jnp.int32(0)
            for slot in range(cap):
                take = (direction[slot] == wanted) & (rank[slot] == level)
                view = jnp.where(take, fields_ref[slot, 2], view)
                anchor = jnp.where(take, fields_ref[slot, 4], anchor)
            values = jnp.where(lane8 == 2 * level, view, values)
            values = jnp.where(lane8 == 2 * level + 1, anchor, values)
        request[side] = values

    pl.semaphore_wait(barrier, slab_count - 1)

    def list_copy(side):
        return pltpu.make_async_remote_copy(
            src_ref=request.at[side],
            dst_ref=asked.at[1 - side],
            send_sem=list_send.at[side],
            recv_sem=list_recv.at[1 - side],
            device_id={"slab": peers[side]},
            device_id_type=pl.DeviceIdType.MESH,
        )

    def list_arrival(side):
        return pltpu.make_async_remote_copy(
            src_ref=request.at[side],
            dst_ref=asked.at[side],
            send_sem=list_send.at[side],
            recv_sem=list_recv.at[side],
            device_id={"slab": peers[side]},
            device_id_type=pl.DeviceIdType.MESH,
        )

    for side in range(2):
        on(side, lambda side=side: list_copy(side).start())

    for copy in small[2:]:
        copy.wait()
    rows = lax.broadcasted_iota(jnp.int32, (lanes_all, lanes_all), 0)

    def fill(table, starts):
        for piece in range(4):
            where = pl.ds(piece * lanes_all, lanes_all)
            start = starts[piece % 2]
            inside = (rows >= start) & (rows < start + edge)
            for side in range(2):
                cols = pl.ds(side * lanes_all, lanes_all)
                table[where, cols] = jnp.where(inside, tx[where, cols], 0.0).astype(jnp.bfloat16)

    for batch in range(batches):
        fill(table_a.at[batch], column[1][2 * batch : 2 * batch + 2])
        for part_z in range(2):
            fill(
                table_b.at[batch, part_z],
                [
                    jnp.where(column[3][spot] == 0, column[4][spot], part_z * edge)
                    for spot in range(2 * batch, 2 * batch + 2)
                ],
            )

    for side in range(2):
        on(side, lambda side=side: list_arrival(side).wait_recv())
    for copy in loads:
        copy.wait()

    def pack_piece(side, level, piece):
        view = asked[side, 0, 2 * level]
        anchor = asked[side, 0, 2 * level + 1]

        def step(index, _):
            z = bounds[piece] + index
            lanes = lax.broadcasted_iota(jnp.int32, (edge, lanes_all), 1)
            low = lanes < edge
            first = held[view, z].astype(jnp.float32)
            second = held[view, half + z].astype(jnp.float32)
            straight = jnp.where(low, first, second)
            turned = pltpu.roll(jnp.where(low, second, first), edge, 1)
            keep = (low & (lanes >= anchor)) | ((lanes >= edge) & (lanes < edge + anchor))
            packed[level][side, z] = jnp.where(keep, straight, turned).astype(jnp.bfloat16)
            return 0

        lax.fori_loop(0, cells[piece], step, 0, unroll=True)

    def block_copy(side, level, piece):
        where = pl.ds(bounds[piece], cells[piece])
        peer = lax.rem(own + slab_count + 2 * side - 1, slab_count)
        return pltpu.make_async_remote_copy(
            src_ref=packed[level].at[side, where],
            dst_ref=got[level][piece].at[side],
            send_sem=send_sems.at[side, level, piece],
            recv_sem=recv_sems.at[side, level, piece],
            device_id={"slab": peer},
            device_id_type=pl.DeviceIdType.MESH,
        )

    def block_arrival(side, level, piece):
        where = pl.ds(bounds[piece], cells[piece])
        return pltpu.make_async_remote_copy(
            src_ref=packed[level].at[side, where],
            dst_ref=got[level][piece].at[1 - side],
            send_sem=send_sems.at[side, level, piece],
            recv_sem=recv_sems.at[1 - side, level, piece],
            device_id={"slab": peers[side]},
            device_id_type=pl.DeviceIdType.MESH,
        )

    items = [
        (side, level, piece)
        for level in range(NBR)
        for piece in range(PIECES)
        for side in range(2)
    ]
    away = lax.rem(own, 2)
    odd = lax.rem(own, 4) * (3 - lax.rem(own, 4)) == 0
    there = (
        jnp.where(away == 0, present[0], present[1]),
        jnp.where(away == 0, present[1], present[0]),
    )

    def send(turn, level, piece):
        side = away if turn == 0 else 1 - away
        pl.when(there[turn])(lambda: block_copy(side, level, piece).start())

    def send_later(moment):
        for turn in range(2):
            late_here = odd & (turn == 0)

            @pl.when(there[turn] & (late_here if moment else jnp.logical_not(late_here)))
            def _(turn=turn):
                side = away if turn == 0 else 1 - away
                for level in range(1, NBR):
                    for piece in range(PIECES):
                        block_copy(side, level, piece).start()

    def pack_level(level, start):
        mine = [(turn, level, piece) for turn in range(2) for piece in range(PIECES)]
        for number, (turn, _, piece) in enumerate(mine):
            pack_piece(away if turn == 0 else 1 - away, level, piece)
            if number and start:
                send(*mine[number - 1])
        if start:
            send(*mine[-1])

    pack_level(0, True)

    lanes = lax.broadcasted_iota(jnp.int32, (edge, lanes_all), 1)
    low = lanes < edge

    def x_planes(left, right, table, z, planes):
        sides = jnp.concatenate(
            [
                left.reshape(planes * edge, lanes_all),
                right.reshape(planes * edge, lanes_all),
            ],
            axis=1,
        )
        mixed = jnp.dot(
            jnp.concatenate([sides, sides], axis=1), table, preferred_element_type=jnp.float32
        )
        high, rest = split(mixed)
        where = pl.ds(z * edge, planes * edge)
        for side in range(2):
            cols = slice(side * lanes_all, (side + 1) * lanes_all)
            x_high[side, where, :] = high[:, cols]
            x_rest[side, where, :] = rest[:, cols]

    def y_planes(z, planes):
        def planar(ref, side):
            return jnp.concatenate(
                [ref[side, pl.ds((z + k) * edge, edge), :] for k in range(planes)], axis=1
            )

        highs = [planar(x_high, 0), planar(x_high, 1)]
        rests = [planar(x_rest, 0), planar(x_rest, 1)]
        mixed = jnp.dot(
            ty[...],
            jnp.concatenate(highs + highs + rests, axis=0),
            preferred_element_type=jnp.float32,
        )
        for index in range(planes):
            where = slice(index * lanes_all, (index + 1) * lanes_all)
            spots = pl.ds(z + index, half + 1, stride=pitch)
            y_re[spots, :] = mixed[: half + 1, where]
            y_im[spots, :] = mixed[kept : kept + half + 1, where]

    def z_plane(ky):
        where = pl.ds(ky * pitch, edge)
        real = split(y_re[where, :])
        imag = split(y_im[where, :])
        return [real[0], imag[0], real[0], imag[0], real[1], imag[1]]

    def z_planes(kys):
        stacks = [z_plane(ky) for ky in kys]
        mixed = jnp.dot(
            tz[...],
            jnp.concatenate(
                [jnp.concatenate([s[k] for s in stacks], axis=1) for k in range(6)], axis=0
            ),
            preferred_element_type=jnp.float32,
        )
        return [
            (
                mixed[:edge, k * lanes_all : (k + 1) * lanes_all],
                mixed[edge:, k * lanes_all : (k + 1) * lanes_all],
            )
            for k in range(len(kys))
        ]

    chunk = edge // 4
    for batch in range(batches):
        views_a = column[0][2 * batch : 2 * batch + 2]

        def first_x(step, batch=batch, views_a=views_a):
            z = chunk * step
            x_planes(
                held[views_a[0], pl.ds(z, chunk)],
                held[views_a[1], pl.ds(z, chunk)],
                table_a[batch],
                z,
                chunk,
            )

        def first_step(step, _, first_x=first_x):
            y_planes(chunk * step, chunk)
            first_x(step + 1)
            return 0

        first_x(0)
        lax.fori_loop(0, edge // chunk - 1, first_step, 0)
        y_planes(edge - chunk, chunk)

        def first_z(step, _, batch=batch):
            for ky, (real, imag) in zip(
                (2 * step, 2 * step + 1), z_planes((2 * step, 2 * step + 1))
            ):
                a_re[batch, ky] = real
                a_im[batch, ky] = imag
            return 0

        lax.fori_loop(0, half // 2, first_z, 0, unroll=4)
        ((real, imag),) = z_planes((half,))
        a_re[batch, half] = real
        a_im[batch, half] = imag
        if batch == 0:
            for level in range(1, NBR):
                pack_level(level, False)

    send_later(0)

    g_re[pl.ds((half + 1) * WIN, (kept - half - 1) * WIN), :] = jnp.zeros(
        ((kept - half - 1) * WIN, lanes_all), jnp.float32
    )
    g_im[pl.ds((half + 1) * WIN, (kept - half - 1) * WIN), :] = jnp.zeros(
        ((kept - half - 1) * WIN, lanes_all), jnp.float32
    )

    total_cells = float(WIN**3)
    found = []
    shift_all = jnp.zeros(shift_ref.shape, jnp.float32)
    sums_all = jnp.zeros(part.shape, jnp.float32)

    for batch in range(batches):
        spots = (2 * batch, 2 * batch + 1)
        local = [column[3][spot] == 0 for spot in spots]
        which = [jnp.where(column[3][spot] < 0, 1, 0) for spot in spots]

        def second(q, piece, part_z, spots=spots, local=local, which=which, batch=batch):
            start = part_z * half + bounds[piece]
            inner = held[column[2][spots[q]], pl.ds(start, cells[piece])]
            outer = got[0][piece][which[q]]
            if batch:
                outer = jnp.where(ranks[spots[q]] > 0, got[1][piece][which[q]], outer)
            return jnp.where(local[q], inner, outer)

        for piece in range(PIECES):
            for side in range(2):
                on(
                    side,
                    lambda side=side, piece=piece: block_arrival(side, batch, piece).wait_recv(),
                )
            for part_z in range(2):
                x_planes(
                    second(0, piece, part_z),
                    second(1, piece, part_z),
                    table_b[batch, part_z],
                    part_z * half + bounds[piece],
                    cells[piece],
                )
            for part_z in range(2):
                if piece:
                    y_planes(part_z * half + bounds[piece - 1], cells[piece - 1])
            if batch == 0 and piece == PIECES - 3:
                send_later(1)
        for part_z in range(2):
            y_planes(part_z * half + bounds[PIECES - 1], cells[PIECES - 1])

        def cross_plane(ky, real, imag, total, batch=batch):
            front_re, front_im = a_re[batch, ky], a_im[batch, ky]
            cross_re = front_re * real + front_im * imag
            cross_im = front_im * real - front_re * imag
            square = cross_re * cross_re + cross_im * cross_im
            size = square * lax.rsqrt(jnp.maximum(square, SMALL))
            c_re[ky] = cross_re
            c_im[ky] = cross_im
            c_abs[ky] = size
            return total + size

        def second_z(step, total, batch=batch):
            kys = (2 * step, 2 * step + 1)
            for ky, (real, imag) in zip(kys, z_planes(kys)):
                total = cross_plane(ky, real, imag, total)
            return total

        total = lax.fori_loop(
            0, half // 2, second_z, jnp.zeros((edge, lanes_all), jnp.float32), unroll=8
        )
        ((real, imag),) = z_planes((half,))
        total = 2.0 * cross_plane(half, real, imag, total) - c_abs[0] - c_abs[half]
        floors = [
            jnp.sum(jnp.where(mask, total, 0.0)) / float(edge**3) + EPSILON
            for mask in (low, jnp.logical_not(low))
        ]
        floor = jnp.where(low, floors[0], floors[1])

        def row_of(value):
            return lax.rem(value + 4 * edge, edge)

        def window_rows(ref, start, first, last):
            return jnp.concatenate(
                [ref[k, pl.ds(start, WIN), :] for k in range(first, last)], axis=1
            )

        wide = wz.shape[0] // 2
        starts = [row_of(column[5][spot]) for spot in spots]
        table_w = jnp.concatenate(
            [
                window_rows(wz, starts[q], kind * wide, (kind + 1) * wide)
                for q in range(2)
                for kind in range(2)
            ],
            axis=0,
        ).astype(jnp.bfloat16)
        low_w = low[:WIN]

        def window_planes(kys, floor=floor, table_w=table_w):
            stacks = []
            for ky in kys:
                size = c_abs[ky] + floor
                inverse = pl.reciprocal(size, approx=True)
                inverse = inverse * (2.0 - size * inverse)
                real = split(c_re[ky] * inverse)
                imag = split(c_im[ky] * inverse)
                stacks.append([real[0], imag[0], real[0], imag[0], real[1], imag[1]])
            mixed = jnp.dot(
                table_w,
                jnp.concatenate(
                    [jnp.concatenate([s[k] for s in stacks], axis=1) for k in range(6)], axis=0
                ),
                preferred_element_type=jnp.float32,
            )
            for k, ky in enumerate(kys):
                cut = mixed[:, k * lanes_all : (k + 1) * lanes_all]
                where = pl.ds(pl.multiple_of(ky * WIN, 8), WIN)
                g_re[where, :] = jnp.where(low_w, cut[:WIN], cut[2 * WIN : 3 * WIN])
                g_im[where, :] = jnp.where(low_w, cut[WIN : 2 * WIN], cut[3 * WIN :])

        def window_step(step, _):
            window_planes((2 * step, 2 * step + 1))
            return 0

        lax.fori_loop(0, half // 2, window_step, 0, unroll=True)
        window_planes((half,))

        stack = jnp.concatenate(
            [
                jnp.concatenate(
                    [ref[pl.ds(i, kept, stride=WIN), :] for i in range(WIN)], axis=1
                )
                for ref in (g_re, g_im)
            ],
            axis=0,
        )
        high, rest = split(stack)
        deep = 6 * kept
        wide = wy.shape[0] // 2
        starts = [row_of(column[6][spot]) for spot in spots]
        table_w = jnp.concatenate(
            [
                window_rows(wy, starts[q], kind * wide, (kind + 1) * wide)
                for q in range(2)
                for kind in range(2)
            ],
            axis=0,
        ).astype(jnp.bfloat16)[:, :deep]
        mixed = jnp.dot(
            table_w,
            jnp.concatenate([high, high, rest], axis=0),
            preferred_element_type=jnp.float32,
        )
        fronts = []
        for kind in range(2):
            pieces = []
            for i in range(WIN):
                where = slice(i * lanes_all, (i + 1) * lanes_all)
                pieces.append(
                    jnp.where(
                        low_w,
                        mixed[kind * WIN : (kind + 1) * WIN, where],
                        mixed[(2 + kind) * WIN : (3 + kind) * WIN, where],
                    )
                )
            fronts.append(jnp.concatenate(pieces, axis=0))
        starts = [row_of(column[7][spot] + column[1][spot] - column[4][spot]) for spot in spots]
        table_w = jnp.concatenate(
            [
                window_rows(wx, starts[q], q * (wx.shape[0] // 2), (q + 1) * (wx.shape[0] // 2))
                for q in range(2)
            ],
            axis=0,
        )
        values = lax.dot_general(
            jnp.concatenate(fronts, axis=1),
            table_w,
            (((1,), (1,)), ((), ())),
            precision=PRECISE,
            preferred_element_type=jnp.float32,
        )
        line = lax.broadcasted_iota(jnp.int32, values.shape, 0)
        lane = lax.broadcasted_iota(jnp.int32, values.shape, 1)
        low_v = lane < WIN
        values = values * jnp.where(
            low_v, alive[spots[0]].astype(jnp.float32), alive[spots[1]].astype(jnp.float32)
        )
        weight = values * values
        places = (line // WIN, line % WIN, lane % WIN)
        found.append(values)
        for q, spot in enumerate(spots):
            mask = low_v if q == 0 else jnp.logical_not(low_v)
            mine = jnp.where(mask, weight, 0.0)
            energy = jnp.sum(mine, keepdims=True) / total_cells
            shifts = [
                (
                    jnp.sum(mine * where.astype(jnp.float32), keepdims=True) / total_cells
                    + energy * column[5 + axis][spot].astype(jnp.float32)
                )
                / (energy + EPSILON)
                for axis, where in enumerate(places)
            ]
            spot_row = lax.broadcasted_iota(jnp.int32, shift_ref.shape, 0)
            spot_lane = lax.broadcasted_iota(jnp.int32, shift_ref.shape, 1)
            for axis in range(3):
                shift_all = jnp.where(
                    (spot_row == axis) & (spot_lane == slots[spot]), shifts[axis], shift_all
                )

            view = lax.broadcasted_iota(jnp.int32, part.shape, 0)
            entry = lax.broadcasted_iota(jnp.int32, part.shape, 1)
            center_z = (own.astype(jnp.float32) * edge + 0.5 * edge) / float(edge * slab_count)
            center_x = (column[1][spot].astype(jnp.float32) + 0.5 * edge) / (2.0 * edge)

            def center(index, center_z=center_z, center_x=center_x):
                return jnp.where(
                    index == 0,
                    center_z,
                    jnp.where(index == 1, 0.5, jnp.where(index == 2, center_x, 1.0)),
                )

            hit_a = (view == column[0][spot]).astype(jnp.float32)
            hit_b = (view == column[2][spot]).astype(jnp.float32)
            block, spot_in = entry // 8, entry % 8
            normal = (hit_a + hit_b) * center(block) * center(spot_in)
            shift = jnp.where(block == 4, shifts[0], jnp.where(block == 5, shifts[1], shifts[2]))
            rhs = (hit_a - hit_b) * center(spot_in) * shift
            sums_all = sums_all + jnp.where(
                block < 4, normal, jnp.where(block < 7, rhs, 0.0)
            ) * (energy / float(cap * slab_count))

    part[...] = sums_all
    shift_ref[...] = shift_all

    def part_copy(peer, source):
        return pltpu.make_async_remote_copy(
            src_ref=part,
            dst_ref=parts.at[source],
            send_sem=sum_send.at[peer],
            recv_sem=sum_recv.at[source],
            device_id={"slab": peer},
            device_id_type=pl.DeviceIdType.MESH,
        )

    def send_part(step, _):
        part_copy(lax.rem(own + step, slab_count), own).start()
        return 0

    lax.fori_loop(1, slab_count, send_part, 0)
    parts[own] = part[...]

    long = corr_ref.shape[1]
    place_row = lax.broadcasted_iota(jnp.int32, (2 * WIN, long), 0)
    place_lane = lax.broadcasted_iota(jnp.int32, (2 * WIN, long), 1)
    spread_row = lax.broadcasted_iota(jnp.int32, (WIN * WIN, long), 0)
    spread_lane = lax.broadcasted_iota(jnp.int32, (WIN * WIN, long), 1)
    slot_row = lax.broadcasted_iota(jnp.int32, corr_ref.shape, 0)
    corr_all = jnp.zeros(corr_ref.shape, jnp.float32)
    for spot in range(cap):
        pick = (place_row == place_lane % WIN + spot % 2 * WIN).astype(jnp.float32)
        spread = jnp.dot(
            found[spot // 2], pick, precision=PRECISE, preferred_element_type=jnp.float32
        )
        row = jnp.sum(
            jnp.where(spread_lane // WIN == spread_row, spread, 0.0), axis=0, keepdims=True
        )
        corr_all = jnp.where(slot_row == slots[spot], row, corr_all)
    corr_ref[...] = corr_all
    for side in range(2):
        on(side, lambda side=side: list_copy(side).wait_send())
    for item in items:
        on(item[0], lambda item=item: block_copy(*item).wait_send())

    def wait_part(step, _):
        peer = lax.rem(own + step, slab_count)
        part_copy(peer, own).wait_send()
        part_copy(peer, peer).wait_recv()
        return 0

    lax.fori_loop(1, slab_count, wait_part, 0)
    sums_ref[...] = jnp.sum(parts[...], axis=0)


def fused(volumes, pair_fields, pair_counts, slab_count):
    views, edge = volumes.shape[0], volumes.shape[1]
    cap = pair_fields.shape[0]
    lanes = 2 * edge
    half = edge // 2
    kept = padded(edge)
    tables = static_tables(edge)
    vmem = pl.BlockSpec(memory_space=pltpu.VMEM)
    hbm = pl.BlockSpec(memory_space=pltpu.HBM)
    f32, bf16 = jnp.float32, jnp.bfloat16
    spectrum = (half + 1, edge, lanes)
    return pl.pallas_call(
        functools.partial(fused_kernel, slab_count),
        out_shape=(
            pltpu.VMEM((cap, WIN**3), f32),
            pltpu.VMEM((8, lanes), f32),
            pltpu.VMEM((views, lanes), f32),
        ),
        in_specs=[hbm] * (3 + len(tables)),
        out_specs=(vmem, vmem, vmem),
        scratch_shapes=[
            pltpu.SMEM(pair_fields.shape, jnp.int32),
            pltpu.SMEM(pair_counts.shape, jnp.int32),
            pltpu.VMEM(volumes.shape, bf16),
        ]
        + [pltpu.VMEM(table.shape, table.dtype) for table in tables]
        + [
            pltpu.VMEM((2, 1, lanes), jnp.int32),
            pltpu.SMEM((2, 1, lanes), jnp.int32),
            pltpu.VMEM((2, half, edge, lanes), bf16),
            pltpu.VMEM((2, half, edge, lanes), bf16),
            pltpu.VMEM((cap // 2, 4 * lanes, 2 * lanes), bf16),
            pltpu.VMEM((cap // 2, 2, 4 * lanes, 2 * lanes), bf16),
            pltpu.VMEM((2, edge * edge, lanes), bf16),
            pltpu.VMEM((2, edge * edge, lanes), bf16),
            pltpu.VMEM((kept * (edge + GAP), lanes), f32),
            pltpu.VMEM((kept * (edge + GAP), lanes), f32),
            pltpu.VMEM((cap // 2,) + spectrum, f32),
            pltpu.VMEM((cap // 2,) + spectrum, f32),
            pltpu.VMEM(spectrum, f32),
            pltpu.VMEM(spectrum, f32),
            pltpu.VMEM(spectrum, f32),
            pltpu.VMEM((kept * WIN, lanes), f32),
            pltpu.VMEM((kept * WIN, lanes), f32),
            pltpu.VMEM((views, lanes), f32),
            pltpu.VMEM((slab_count, views, lanes), f32),
            pltpu.SemaphoreType.DMA((2 + len(tables),)),
            pltpu.SemaphoreType.DMA((LOADS,)),
            pltpu.SemaphoreType.DMA((2,)),
            pltpu.SemaphoreType.DMA((2,)),
            pltpu.SemaphoreType.DMA((2, NBR, PIECES)),
            pltpu.SemaphoreType.DMA((2, NBR, PIECES)),
            pltpu.SemaphoreType.DMA((slab_count,)),
            pltpu.SemaphoreType.DMA((slab_count,)),
        ]
        + [
            pltpu.VMEM((2, last - first, edge, lanes), bf16)
            for first, last in zip(cuts(half), cuts(half)[1:])
        ]
        * NBR,
        compiler_params=pltpu.CompilerParams(
            collective_id=1, has_side_effects=True, vmem_limit_bytes=60 * 2**20
        ),
        name="fused",
    )(pair_fields, pair_counts, volumes, *[jnp.asarray(table) for table in tables])


def finish_kernel(corr_in, shift_in, sums_in, corr_ref, shift_ref, normal_ref, rhs_ref):
    views, lanes = sums_in.shape
    corr_ref[...] = corr_in[...]
    shift_ref[...] = shift_in[: shift_ref.shape[0], : shift_ref.shape[1]]
    turned = jnp.concatenate(
        [sums_in[...], jnp.zeros((lanes - views, lanes), jnp.float32)], axis=0
    ).T
    for index in range(4):
        normal_ref[index] = turned[8 * index : 8 * index + 4, :views]
    for index in range(3):
        rhs_ref[index] = turned[32 + 8 * index : 36 + 8 * index, :views]


def finished(corr, shifts, sums):
    cap, views = corr.shape[0], sums.shape[0]
    vmem = pl.BlockSpec(memory_space=pltpu.VMEM)
    f32 = jnp.float32
    return pl.pallas_call(
        finish_kernel,
        out_shape=(
            jax.ShapeDtypeStruct(corr.shape, f32),
            jax.ShapeDtypeStruct((3, cap), f32),
            jax.ShapeDtypeStruct((4, 4, views), f32),
            jax.ShapeDtypeStruct((3, 4, views), f32),
        ),
        in_specs=[vmem] * 3,
        out_specs=(vmem,) * 4,
        name="finish",
    )(*[pltpu.with_memory_space_constraint(x, pltpu.VMEM) for x in (corr, shifts, sums)])


def on_device(volumes, pair_fields, pair_counts):
    slab_count = lax.axis_size("slab")
    corr, shifts, sums = fused(
        volumes, pair_fields.T, pair_counts.reshape(1, 1), slab_count
    )
    corr, shifts, normal, rhs = finished(corr, shifts, sums)
    return corr, shifts, normal.transpose(2, 0, 1), rhs.transpose(2, 1, 0)


def solution(mesh):
    in_specs = (P("tm", "slab", None, None), P(None, ("tm", "slab")), P(("tm", "slab")))
    out_specs = (
        P(("tm", "slab"), None),
        P(None, ("tm", "slab")),
        P("tm", None, None),
        P("tm", None, None),
    )
    return jax.shard_map(
        on_device, mesh=mesh, in_specs=in_specs, out_specs=out_specs, check_vma=False
    )
```
